8 devices in a mesh: sweep: 1 (over z), data: 2 (over y), ent: 4 (over x, core).
Axes of the slice: x: 2, y: 2, z: 1, core: 2. Of those that a mesh axis runs over, the one named last changes fastest.
Arguments:
- ent_table: float32 [65536, 400], P(('sweep', 'ent'))
- ada_state: float32 [65536], P(('sweep', 'ent'))
- rel_table: float32 [1345, 400], P('sweep')
- head_idx: int32 [4, 2, 4, 8192], P(('sweep', 'ent'), 'data')
- tail_idx: int32 [4, 2, 4, 8192], P(('sweep', 'ent'), 'data')
- rel_idx: int32 [4, 2, 4, 8192], P(('sweep', 'ent'), 'data')
- edge_mask: int32 [4, 2, 4, 8192], P(('sweep', 'ent'), 'data')
- neg_idx: int32 [4, 2, 4, 256], P(('sweep', 'ent'), 'data')
Outputs:
- output 1: float32 [65536, 400], P(('sweep', 'ent'))
- output 2: float32 [65536], P(('sweep', 'ent'))
- output 3: float32 [1345, 400], P('sweep')
- output 4: float32 [4, 2, 4], P(('sweep', 'ent'), 'data')
All inputs are finite; a program needn't handle non-finite values.
Results may differ from the reference program's by a relative error of at most 0.001.
Values are sent between devices in bfloat16 or wider.
A program may use at most 1 GiB of HBM per device.

```python
import jax
import jax.numpy as jnp
from jax import lax

ENT_PARTS = 4
DATA_SHARDS = 2
ENT_ROWS = 16384
DIM = 400
RELS = 1345
NEGS = 256
EDGES = 8192

TOTAL_ROWS = ENT_PARTS * ENT_ROWS
HOT_ROWS = max(ENT_ROWS // 16, 1)
HOT_RELS = max(RELS // 16, 1)
LEARN_ENT = 0.1
LEARN_REL = 0.05
ADA_EPS = 1e-6


def mixed_index(key, idx_shape, full_span, hot_span):
    key_coin, key_hot, key_all = jax.random.split(key, 3)
    coin_flip = jax.random.randint(key_coin, idx_shape, 0, 2)
    hot_pick = jax.random.randint(key_hot, idx_shape, 0, hot_span)
    any_pick = jax.random.randint(key_all, idx_shape, 0, full_span)
    return jnp.where(coin_flip == 1, hot_pick, any_pick).astype(jnp.int32)


def setup_inputs(seed: int = 0, part: int = 0) -> dict:
    base_key = jax.random.fold_in(jax.random.key(seed), part)
    key_list = jax.random.split(base_key, 9)
    ent_scale = (2.0 * DIM) ** -0.25
    edge_shape = (ENT_PARTS, DATA_SHARDS, ENT_PARTS, EDGES)
    fill_level = jax.random.randint(key_list[6], (ENT_PARTS, DATA_SHARDS, ENT_PARTS, 1), 1, 17)
    return {
        "ent_table": jax.random.normal(key_list[0], (TOTAL_ROWS, DIM), jnp.float32) * ent_scale,
        "ada_state": jax.random.uniform(key_list[1], (TOTAL_ROWS,), jnp.float32, 0.5, 2.0) * (ent_scale * ent_scale),
        "rel_table": jax.random.normal(key_list[2], (RELS, DIM), jnp.float32),
        "head_idx": mixed_index(key_list[3], edge_shape, ENT_ROWS, HOT_ROWS),
        "tail_idx": mixed_index(key_list[4], edge_shape, ENT_ROWS, HOT_ROWS),
        "rel_idx": mixed_index(key_list[5], edge_shape, RELS, HOT_RELS),
        "edge_mask": (jax.random.randint(key_list[7], edge_shape, 0, 16) < fill_level).astype(jnp.int32),
        "neg_idx": mixed_index(key_list[8], (ENT_PARTS, DATA_SHARDS, ENT_PARTS, NEGS), ENT_ROWS, HOT_ROWS),
    }


def complex_mul(left, right):
    half_dim = left.shape[-1] // 2
    left_re, left_im = left[..., :half_dim], left[..., half_dim:]
    right_re, right_im = right[..., :half_dim], right[..., half_dim:]
    return jnp.concatenate([left_re * right_re - left_im * right_im, left_re * right_im + left_im * right_re], axis=-1)


def complex_mul_conj(left, right):
    half_dim = left.shape[-1] // 2
    left_re, left_im = left[..., :half_dim], left[..., half_dim:]
    right_re, right_im = right[..., :half_dim], right[..., half_dim:]
    return jnp.concatenate([left_re * right_re + left_im * right_im, left_im * right_re - left_re * right_im], axis=-1)


def bucket_grads(head_rows, tail_rows, neg_rows, rel_rows, weight):
    query_vec = complex_mul(head_rows, rel_rows)
    tail_f32 = tail_rows.astype(jnp.float32)
    pos_score = jnp.sum(query_vec * tail_f32, axis=-1)
    query_bf = query_vec.astype(jnp.bfloat16)
    neg_score = jnp.dot(query_bf, neg_rows.T, preferred_element_type=jnp.float32)
    top_score = jnp.maximum(pos_score, jnp.max(neg_score, axis=-1))
    pos_exp = jnp.exp(pos_score - top_score)
    neg_exp = jnp.exp(neg_score - top_score[:, None])
    norm_sum = pos_exp + jnp.sum(neg_exp, axis=-1)
    loss_sum = jnp.sum(weight * (top_score + jnp.log(norm_sum) - pos_score))
    pos_coef = weight * (pos_exp / norm_sum - 1.0)
    neg_coef = ((weight / norm_sum)[:, None] * neg_exp).astype(jnp.bfloat16)
    query_grad = pos_coef[:, None] * tail_f32 + jnp.dot(neg_coef, neg_rows, preferred_element_type=jnp.float32)
    tail_grad = pos_coef[:, None] * query_vec
    neg_grad = jnp.dot(neg_coef.T, query_bf, preferred_element_type=jnp.float32)
    head_grad = complex_mul_conj(query_grad, rel_rows)
    rel_grad = complex_mul_conj(query_grad, head_rows)
    return head_grad, tail_grad, neg_grad, rel_grad, loss_sum


def reference(ent_table, ada_state, rel_table, head_idx, tail_idx, rel_idx, edge_mask, neg_idx):
    bucket_count = ENT_PARTS * DATA_SHARDS
    head_part = jnp.repeat(jnp.arange(ENT_PARTS, dtype=jnp.int32), DATA_SHARDS)[:, None]

    def one_round(round_carry, round_idx):
        ent_cur, state_cur, rel_cur, rel_state = round_carry
        tail_part = (head_part + round_idx) % ENT_PARTS
        head_ids = head_idx[:, :, round_idx].reshape(bucket_count, EDGES) + head_part * ENT_ROWS
        tail_ids = tail_idx[:, :, round_idx].reshape(bucket_count, EDGES) + tail_part * ENT_ROWS
        neg_ids = neg_idx[:, :, round_idx].reshape(bucket_count, NEGS) + tail_part * ENT_ROWS
        rel_ids = rel_idx[:, :, round_idx].reshape(bucket_count, EDGES)
        weights = edge_mask[:, :, round_idx].reshape(bucket_count, EDGES).astype(jnp.float32)
        table_bf = ent_cur.astype(jnp.bfloat16)

        def one_bucket(acc_carry, bucket):
            row_acc, rel_acc = acc_carry
            bucket_head, bucket_tail, bucket_neg, bucket_rel, bucket_weight = bucket
            head_grad, tail_grad, neg_grad, rel_grad, loss_sum = bucket_grads(
                ent_cur[bucket_head], table_bf[bucket_tail], table_bf[bucket_neg], rel_cur[bucket_rel], bucket_weight)
            row_ids = jnp.concatenate([bucket_head, bucket_tail, bucket_neg])
            row_acc = row_acc.at[row_ids].add(jnp.concatenate([head_grad, tail_grad, neg_grad], axis=0))
            rel_acc = rel_acc.at[bucket_rel].add(rel_grad)
            return (row_acc, rel_acc), loss_sum

        acc_init = (jnp.zeros((TOTAL_ROWS, DIM), jnp.float32), jnp.zeros((RELS, DIM), jnp.float32))
        grad_pair, loss_sums = lax.scan(one_bucket, acc_init, (head_ids, tail_ids, neg_ids, rel_ids, weights))
        row_grad, rel_grad = grad_pair
        state_cur = state_cur + jnp.mean(row_grad * row_grad, axis=-1)
        ent_cur = ent_cur - LEARN_ENT * row_grad / jnp.sqrt(state_cur + ADA_EPS)[:, None]
        rel_state = rel_state + jnp.mean(rel_grad * rel_grad, axis=-1)
        rel_cur = rel_cur - LEARN_REL * rel_grad / jnp.sqrt(rel_state + ADA_EPS)[:, None]
        return (ent_cur, state_cur, rel_cur, rel_state), loss_sums.reshape(ENT_PARTS, DATA_SHARDS) / EDGES

    carry_init = (ent_table, ada_state, rel_table, jnp.zeros((RELS,), jnp.float32))
    carry_end, round_loss = lax.scan(one_round, carry_init, jnp.arange(ENT_PARTS, dtype=jnp.int32))
    return (carry_end[0], carry_end[1], carry_end[2], jnp.transpose(round_loss, (1, 2, 0)))
```

```python
import functools

import jax
import jax.numpy as jnp
from jax import lax
from jax.experimental import pallas as pl
from jax.experimental.pallas import tpu as pltpu
from jax.sharding import PartitionSpec as P


LEARN_ENT = 0.1
LEARN_REL = 0.05
ADA_EPS = 1e-6

CH = 4
LANE = 128
BLK = 512
GROUP = 16
REL_GROUP = 8
UNROLL = 8
WBLK = 1024
PIECES = 2
VMEM_LIMIT = 64 * 1024 * 1024 - 65536
F32 = jnp.float32
BF16 = jnp.bfloat16


def params():
    return pltpu.CompilerParams(dimension_semantics=("arbitrary",), vmem_limit_bytes=VMEM_LIMIT)


def cost(flops, bytes_accessed):
    return pl.CostEstimate(flops=flops, bytes_accessed=bytes_accessed, transcendentals=0)


def row_at(n):
    return pl.ds(pl.multiple_of(n * CH, CH), CH)


def id_row(ids, at, leads, off=0):
    value = ids.at[pl.ds(at, off + 1)][off]
    return pl.ds(pl.multiple_of(value & -CH if leads else value, CH), CH)


def mark_groups(ids, size):
    count = ids.shape[-1]
    place = lax.broadcasted_iota(jnp.int32, ids.shape, ids.ndim - 1) % size
    hit = jnp.zeros(ids.shape, jnp.int32)
    for k in range(1, size):
        hit = hit | ((ids == jnp.roll(ids, k, axis=-1)) & (place >= k)).astype(jnp.int32)
    k = 1
    while k < size:
        hit = hit | jnp.roll(hit, -k, axis=-1)
        k *= 2
    return ids * CH + jnp.where(place == 0, hit, 0)


def chunk(buf, j, count, base=0):
    return buf[pl.ds(base * CH + j, count, stride=CH), :]


def put_chunk(buf, j, count, val, base=0):
    buf[pl.ds(base * CH + j, count, stride=CH), :] = val


def pack_rows(x):
    rows, dim = x.shape
    half = dim // 2
    x = jnp.pad(x.reshape(rows, 2, half), ((0, 0), (0, 0), (0, 2 * LANE - half)))
    return x.reshape(rows * CH, LANE)


def unpack_rows(x, dim):
    rows = x.shape[0] // CH
    return x.reshape(rows, 2, 2 * LANE)[:, :, :dim // 2].reshape(rows, dim)


def wire_rows(dim, dtype):
    half = dim // 2
    rest = half - LANE
    if dtype == F32:
        return [(0, LANE, LANE), (LANE, rest, rest), (half, LANE, LANE), (half + LANE, rest, rest)], dim
    step = -(-rest // 16) * 16
    return [(0, LANE, LANE), (2 * LANE, step, step), (LANE, LANE, LANE), (2 * LANE + step, step, step)], 2 * LANE + 2 * step


def wire_get(ref, lanes, j, dim):
    off, size, _ = wire_rows(dim, ref.dtype)[0][j]
    x = ref[pl.ds(off, size), lanes].astype(F32)
    if size < LANE:
        x = jnp.concatenate([x, jnp.zeros((LANE - size, LANE), F32)], axis=0)
    return x.T


def wire_put(ref, lanes, j, dim, val):
    off, size, _ = wire_rows(dim, ref.dtype)[0][j]
    ref[pl.ds(off, size), lanes] = val.T[:size].astype(ref.dtype)


def clip_piece(t, p, per):
    return jnp.clip(t - p * per, 0, per - 1)


def row_block(t, mine, blocks):
    half = blocks // 2
    return jnp.where(t < half, mine * half + t, (1 - mine) * half + t - half)


def gather_rows(ids, base, table, buf, count):
    def body(t, carry):
        e = t * UNROLL
        for u in range(UNROLL):
            buf[row_at(e + u), :] = table[id_row(ids, base + e, u == 0, u), :]
        return carry
    lax.fori_loop(0, count // UNROLL, body, 0)


def group_rows(ids, at, size, lead):
    return [id_row(ids, at, g % lead == 0, g) for g in range(size)]


def add_one(row, e, buf, acc):
    acc[row, :] += buf[row_at(e), :]


def add_group(at, e, buf, acc):
    total = [acc[row, :] + buf[row_at(e + g), :] for g, row in enumerate(at)]
    for row, value in zip(at, total):
        acc[row, :] = value


def scatter_rows(ids, base, buf, acc, count):
    def body(t, carry):
        e = t * GROUP

        def fast():
            add_group(group_rows(ids, base + e, GROUP, GROUP), e, buf, acc)

        def slow():
            for g, row in enumerate(group_rows(ids, base + e, GROUP, GROUP)):
                add_one(row, e + g, buf, acc)

        lax.cond((ids[base + e] & 1) == 0, fast, slow)
        return carry
    lax.fori_loop(0, count // GROUP, body, 0)


def scatter_plain(ids, buf, acc, count):
    def body(t, carry):
        e = t * UNROLL
        for u, row in enumerate(group_rows(ids, e, UNROLL, UNROLL)):
            add_one(row, e + u, buf, acc)
        return carry
    lax.fori_loop(0, count // UNROLL, body, 0)


def zero_rows(acc):
    rows = acc.shape[0]
    size = 512

    def body(t, carry):
        acc[pl.ds(pl.multiple_of(t * size, size), size), :] = jnp.zeros((size, LANE), F32)
        return carry
    full = rows // size
    lax.fori_loop(0, full, body, 0)
    if rows % size:
        acc[full * size:, :] = jnp.zeros((rows % size, LANE), F32)


def block_live(step, steps, cnt):
    return (step % steps) * BLK < cnt[step // steps]


def edge_block(i, steps, cnt):
    shard = i // steps
    last = jnp.maximum((cnt[shard] + (BLK - 1)) // BLK - 1, 0)
    return shard * steps + jnp.minimum(i % steps, last)


def run_copy(src, dst, sem):
    copy = pltpu.make_async_copy(src, dst, sem)
    copy.start()
    copy.wait()


def pack_kernel(dim, x_ref, out_ref):
    for r in range(WBLK // LANE):
        for j in range(CH):
            put_chunk(out_ref, j, LANE, wire_get(x_ref, pl.ds(r * LANE, LANE), j, dim), r * LANE)


def pack_call(x):
    dim, rows = x.shape
    return pl.pallas_call(
        functools.partial(pack_kernel, dim),
        grid=(rows // WBLK,),
        in_specs=[pl.BlockSpec((dim, WBLK), lambda i: (0, i))],
        out_specs=pl.BlockSpec((CH * WBLK, LANE), lambda i: (i, 0)),
        out_shape=jax.ShapeDtypeStruct((CH * rows, LANE), F32),
        compiler_params=params(), cost_estimate=cost(rows, rows * 4096), name="pack",
    )(x)


def query_kernel(steps, cnt, hid, rid, ent_hbm, rel_ref, q_ref, a_ref, ent, abuf, rbuf, sem):
    step = pl.program_id(0)

    @pl.when(step == 0)
    def _():
        run_copy(ent_hbm, ent, sem)

    @pl.when(block_live(step, steps, cnt))
    def _():
        base = step * BLK

        def body(t, carry):
            e = t * UNROLL
            for u in range(UNROLL):
                abuf[row_at(e + u), :] = ent[id_row(hid, base + e, u == 0, u), :]
                rbuf[row_at(e + u), :] = rel_ref[id_row(rid, base + e, u == 0, u), :]
            return carry
        lax.fori_loop(0, BLK // UNROLL, body, 0)
        for j in range(2):
            a_re, a_im = chunk(abuf, j, BLK), chunk(abuf, j + 2, BLK)
            r_re, r_im = chunk(rbuf, j, BLK), chunk(rbuf, j + 2, BLK)
            q_ref[j] = a_re * r_re - a_im * r_im
            q_ref[j + 2] = a_re * r_im + a_im * r_re
            a_ref[j] = a_re
            a_ref[j + 2] = a_im


def query_call(cnt, hid, rid, ent, rel):
    edges = hid.shape[0]
    steps = edges // cnt.shape[0] // BLK
    edge_spec = pl.BlockSpec((CH, BLK, LANE), lambda i, cnt, *_: (0, edge_block(i, steps, cnt), 0))
    return pl.pallas_call(
        functools.partial(query_kernel, steps),
        grid_spec=pltpu.PrefetchScalarGridSpec(
            num_scalar_prefetch=3,
            grid=(edges // BLK,),
            in_specs=[
                pl.BlockSpec(memory_space=pl.ANY),
                pl.BlockSpec(rel.shape, lambda i, *_: (0, 0)),
            ],
            out_specs=[edge_spec] * 2,
            scratch_shapes=[
                pltpu.VMEM(ent.shape, F32),
                pltpu.VMEM((BLK * CH, LANE), F32),
                pltpu.VMEM((BLK * CH, LANE), F32),
                pltpu.SemaphoreType.DMA,
            ],
        ),
        out_shape=[jax.ShapeDtypeStruct((CH, edges, LANE), F32)] * 2,
        compiler_params=params(), cost_estimate=cost(edges * 3000, edges * 6144), name="query",
    )(cnt, hid, rid, ent, rel)


def main_kernel(steps, loads, wired, kinds, dim, flags, cnt, tid, nid, *refs):
    parts = {}
    refs = list(refs)
    if wired:
        for kind in kinds:
            parts[kind] = [refs.pop(0) for _ in range(PIECES)]
    else:
        ent_hbm = refs.pop(0)
    q_ref, dq_ref, tg_ref, neg_ref, loss_ref, ent, cbuf, mbuf, nacc = refs[:9]
    at = pl.program_id(0)
    negs = mbuf.shape[0]

    if wired:
        per = loads // (2 * PIECES)
        mine, near = flags[0], flags[1]

        def fill(ref):
            base = row_block(at, mine, loads) * WBLK

            def body(r, carry):
                lanes = pl.ds(pl.multiple_of(r * LANE, LANE), LANE)
                for j in range(CH):
                    put_chunk(ent, j, LANE, wire_get(ref, lanes, j, dim), base + r * LANE)
                return carry
            lax.fori_loop(0, WBLK // LANE, body, 0, unroll=True)

        for p in range(PIECES):
            pl.when(at // per == p)(functools.partial(fill, parts["first"][p]))
            late = at // per == PIECES + p
            if "second" in kinds:
                pl.when(late & (near == 0))(functools.partial(fill, parts["second"][p]))
            if "direct" in kinds:
                pl.when(late & (near == 1))(functools.partial(fill, parts["direct"][p]))
    else:
        @pl.when(at == 0)
        def _():
            run_copy(ent_hbm, ent, refs[9])

    step = jnp.maximum(at - loads, 0)
    shard = step // steps
    live = at >= loads

    @pl.when(live & (step % steps == 0))
    def _():
        for start in range(0, negs, min(BLK, negs)):
            gather_rows(nid, shard * negs + start, ent, cbuf, min(BLK, negs))
            for j in range(CH):
                mbuf[pl.ds(start, min(BLK, negs)), pl.ds(j * LANE, LANE)] = chunk(cbuf, j, min(BLK, negs)).astype(BF16)
        nacc[...] = jnp.zeros_like(nacc)
        loss_ref[...] = jnp.zeros_like(loss_ref)

    @pl.when(live & block_live(step, steps, cnt))
    def _():
        gather_rows(tid, step * BLK, ent, cbuf, BLK)
        c = [chunk(cbuf, j, BLK).astype(BF16).astype(F32) for j in range(CH)]
        q = [q_ref[j] for j in range(CH)]
        p = jnp.sum(q[0] * c[0] + q[1] * c[1] + q[2] * c[2] + q[3] * c[3], axis=1, keepdims=True)
        q_bf = jnp.concatenate([x.astype(BF16) for x in q], axis=1)
        m = mbuf[...]
        s = lax.dot_general(q_bf, m, (((1,), (1,)), ((), ())), preferred_element_type=F32)
        place = lax.broadcasted_iota(jnp.int32, (BLK, 1), 0) + (step % steps) * BLK
        w = jnp.where(place < cnt[shard], 1.0, 0.0)
        top = jnp.maximum(p, jnp.max(s, axis=1, keepdims=True))
        p_exp = jnp.exp(p - top)
        n_exp = jnp.exp(s - top)
        norm = p_exp + jnp.sum(n_exp, axis=1, keepdims=True)
        loss = jnp.sum(w * (top + jnp.log(norm) - p), axis=0, keepdims=True)
        loss_ref[...] += jnp.broadcast_to(loss[None], loss_ref.shape)
        alpha = w * (p_exp / norm - 1.0)
        beta = ((w / norm) * n_exp).astype(BF16)
        back = jnp.dot(beta, m, preferred_element_type=F32)
        for j in range(CH):
            dq_ref[j] = alpha * c[j] + back[:, j * LANE:(j + 1) * LANE]
            put_chunk(tg_ref, j, BLK, alpha * q[j])
        nacc[...] += lax.dot_general(beta, q_bf, (((0,), (0,)), ((), ())), preferred_element_type=F32)

    @pl.when(live & (step % steps == steps - 1))
    def _():
        for j in range(CH):
            put_chunk(neg_ref, j, negs, nacc[:, j * LANE:(j + 1) * LANE])


def wire_in_specs(kinds, width, blocks, shift=0):
    per = blocks // (2 * PIECES)
    specs = []
    for kind in kinds:
        for p in range(PIECES):
            def index(i, flags, *_, kind=kind, p=p):
                if kind == "first":
                    return 0, clip_piece(i + shift, p, per)
                used = flags[1] if kind == "direct" else 1 - flags[1]
                return 0, clip_piece(i + shift, PIECES + p, per) * used
            specs.append(pl.BlockSpec((width, WBLK), index))
    return specs


def main_call(flags, cnt, tid, nid, tails, q, rows, dim):
    edges = tid.shape[0]
    shards = cnt.shape[0]
    negs = nid.shape[0] // shards
    steps = edges // shards // BLK
    wired = isinstance(tails, dict)
    if wired:
        loads, kinds = rows // WBLK, list(tails)
        operands = [x for kind in kinds for x in tails[kind]]
        specs = wire_in_specs(kinds, operands[0].shape[0], loads)
        sems = []
    else:
        loads, kinds, operands, specs = 0, [], [tails], [pl.BlockSpec(memory_space=pl.ANY)]
        sems = [pltpu.SemaphoreType.DMA]

    def block(i, cnt):
        return edge_block(jnp.maximum(i - loads, 0), steps, cnt)

    def shard_of(i):
        return jnp.maximum(i - loads, 0) // steps

    edge_spec = pl.BlockSpec((CH, BLK, LANE), lambda i, flags, cnt, *_: (0, block(i, cnt), 0))
    return pl.pallas_call(
        functools.partial(main_kernel, steps, loads, wired, kinds, dim),
        grid_spec=pltpu.PrefetchScalarGridSpec(
            num_scalar_prefetch=4,
            grid=(loads + edges // BLK,),
            in_specs=specs + [edge_spec],
            out_specs=[
                edge_spec,
                pl.BlockSpec((CH * BLK, LANE), lambda i, flags, cnt, *_: (block(i, cnt), 0)),
                pl.BlockSpec((CH * negs, LANE), lambda i, *_: (shard_of(i), 0)),
                pl.BlockSpec((1, 8, LANE), lambda i, *_: (shard_of(i), 0, 0)),
            ],
            scratch_shapes=[
                pltpu.VMEM((CH * rows, LANE), F32),
                pltpu.VMEM((BLK * CH, LANE), F32),
                pltpu.VMEM((negs, CH * LANE), BF16),
                pltpu.VMEM((negs, CH * LANE), F32),
            ] + sems,
        ),
        out_shape=[
            jax.ShapeDtypeStruct((CH, edges, LANE), F32),
            jax.ShapeDtypeStruct((CH * edges, LANE), F32),
            jax.ShapeDtypeStruct((CH * negs * shards, LANE), F32),
            jax.ShapeDtypeStruct((shards, 8, LANE), F32),
        ],
        compiler_params=params(), cost_estimate=cost(edges * negs * 3072, edges * 8192), name="scores",
    )(flags, cnt, tid, nid, *operands, q)


def tail_kernel(steps, total, blocks, dim, flags, cnt, tid, nid, tg_ref, neg_ref, *refs):
    step = pl.program_id(0)
    acc = refs[-1]

    @pl.when(step == 0)
    def _():
        zero_rows(acc)
        scatter_plain(nid, neg_ref, acc, nid.shape[0])

    @pl.when((step < total) & block_live(jnp.minimum(step, total - 1), steps, cnt))
    def _():
        scatter_rows(tid, step * BLK, tg_ref, acc, BLK)

    outs = refs[:-1]
    per = blocks // (2 * PIECES)
    at = step - total

    def emit(ref):
        base = row_block(at, flags[0], blocks) * WBLK

        def body(r, carry):
            lanes = pl.ds(pl.multiple_of(r * LANE, LANE), LANE)
            for j in range(CH):
                wire_put(ref, lanes, j, dim, chunk(acc, j, LANE, base + r * LANE))
            return carry
        lax.fori_loop(0, WBLK // LANE, body, 0, unroll=True)

    for p, ref in enumerate(outs):
        pl.when((at >= 0) & (at // per == p))(functools.partial(emit, ref))


def tail_call(flags, cnt, tid, nid, tg, neg, rows, dim, near):
    edges = tid.shape[0]
    total = edges // BLK
    steps = total // cnt.shape[0]
    blocks = rows // WBLK
    per = blocks // (2 * PIECES)
    acc = pltpu.VMEM((CH * rows, LANE), F32)
    pieces = PIECES * (2 if near else 1)
    grid = total + pieces * per
    out_specs = [
        pl.BlockSpec((dim, WBLK), lambda i, *_, p=p: (0, clip_piece(i - total, p, per))) for p in range(pieces)]
    out_shape = [jax.ShapeDtypeStruct((dim, per * WBLK), F32)] * pieces
    scratch = [acc]
    return pl.pallas_call(
        functools.partial(tail_kernel, steps, total, blocks, dim),
        grid_spec=pltpu.PrefetchScalarGridSpec(
            num_scalar_prefetch=4,
            grid=(grid,),
            in_specs=[
                pl.BlockSpec((CH * BLK, LANE),
                             lambda i, flags, cnt, *_: (edge_block(jnp.minimum(i, total - 1), steps, cnt), 0)),
                pl.BlockSpec(neg.shape, lambda i, *_: (0, 0)),
            ],
            out_specs=out_specs,
            scratch_shapes=scratch,
        ),
        out_shape=out_shape,
        compiler_params=params(), cost_estimate=cost(edges * 3000, edges * 6144), name="tails",
    )(flags, cnt, tid, nid, tg, neg)


def head_kernel(steps, both, cnt, hid, rid, *refs):
    refs = list(refs)
    if both:
        tid, nid = refs.pop(0), refs.pop(0)
        tg_ref, neg_ref = refs.pop(0), refs.pop(0)
    rel_ref, dq_ref, a_ref, out_hbm, racc_hbm, acc, racc, rbuf, hbuf, gbuf, sem, rsem = refs
    step = pl.program_id(0)

    @pl.when(step == 0)
    def _():
        zero_rows(acc)
        zero_rows(racc)
        if both:
            scatter_plain(nid, neg_ref, acc, nid.shape[0])

    @pl.when(block_live(step, steps, cnt))
    def _():
        base = step * BLK
        gather_rows(rid, base, rel_ref, rbuf, BLK)
        for j in range(2):
            d_re, d_im = dq_ref[j], dq_ref[j + 2]
            r_re, r_im = chunk(rbuf, j, BLK), chunk(rbuf, j + 2, BLK)
            put_chunk(hbuf, j, BLK, d_re * r_re + d_im * r_im)
            put_chunk(hbuf, j + 2, BLK, d_im * r_re - d_re * r_im)
            a_re, a_im = a_ref[j], a_ref[j + 2]
            put_chunk(gbuf, j, BLK, d_re * a_re + d_im * a_im)
            put_chunk(gbuf, j + 2, BLK, d_im * a_re - d_re * a_im)

        def body(t, carry):
            e = t * GROUP
            repeat = hid[base + e]
            for g in range(0, GROUP, REL_GROUP):
                repeat = repeat | rid[base + e + g]

            def fast():
                add_group(group_rows(hid, base + e, GROUP, GROUP), e, hbuf, acc)
                for g in range(0, GROUP, REL_GROUP):
                    add_group(group_rows(rid, base + e + g, REL_GROUP, REL_GROUP), e + g, gbuf, racc)

            def slow():
                for g in range(GROUP):
                    add_one(id_row(hid, base + e, g == 0, g), e + g, hbuf, acc)
                    add_one(id_row(rid, base + e, g % REL_GROUP == 0, g), e + g, gbuf, racc)

            lax.cond((repeat & 1) == 0, fast, slow)
            return carry
        lax.fori_loop(0, BLK // GROUP, body, 0)
        if both:
            scatter_rows(tid, base, tg_ref, acc, BLK)

    @pl.when(step == pl.num_programs(0) - 1)
    def _():
        copy = pltpu.make_async_copy(acc, out_hbm, sem)
        copy.start()
        rcopy = pltpu.make_async_copy(racc, racc_hbm, rsem)
        rcopy.start()
        copy.wait()
        rcopy.wait()


def head_call(cnt, hid, rid, rel, dq, a, rows, tails=None):
    edges = hid.shape[0]
    steps = edges // cnt.shape[0] // BLK
    both = tails is not None
    scalars, operands, specs = [cnt, hid, rid], [], []
    if both:
        tid, nid, tg, neg = tails
        scalars += [tid, nid]
        operands = [tg, neg]
        specs = [pl.BlockSpec((CH * BLK, LANE), lambda i, cnt, *_: (edge_block(i, steps, cnt), 0)),
                 pl.BlockSpec(neg.shape, lambda i, *_: (0, 0))]
    edge_spec = pl.BlockSpec((CH, BLK, LANE), lambda i, cnt, *_: (0, edge_block(i, steps, cnt), 0))
    return pl.pallas_call(
        functools.partial(head_kernel, steps, both),
        grid_spec=pltpu.PrefetchScalarGridSpec(
            num_scalar_prefetch=len(scalars),
            grid=(edges // BLK,),
            in_specs=specs + [pl.BlockSpec(rel.shape, lambda i, *_: (0, 0)), edge_spec, edge_spec],
            out_specs=[pl.BlockSpec(memory_space=pl.ANY)] * 2,
            scratch_shapes=[
                pltpu.VMEM((CH * rows, LANE), F32),
                pltpu.VMEM(rel.shape, F32),
                pltpu.VMEM((BLK * CH, LANE), F32),
                pltpu.VMEM((BLK * CH, LANE), F32),
                pltpu.VMEM((BLK * CH, LANE), F32),
                pltpu.SemaphoreType.DMA,
                pltpu.SemaphoreType.DMA,
            ],
        ),
        out_shape=[jax.ShapeDtypeStruct((CH * rows, LANE), F32), jax.ShapeDtypeStruct(rel.shape, F32)],
        compiler_params=params(), cost_estimate=cost(edges * 6000, edges * 8192), name="heads",
    )(*scalars, *operands, rel, dq, a)


def update_kernel(dim, blocks, kinds, outs, final, flags, *refs):
    refs = list(refs)
    parts = {kind: [refs.pop(0) for _ in range(PIECES)] for kind in kinds}
    ent_ref, head_ref, state_ref = refs[:3]
    if final == "late":
        refs.pop(3)
    new_ref, new_state = refs[3:5]
    wires = refs[5:]
    at = pl.program_id(0)
    per = blocks // (2 * PIECES)
    near = flags[1]
    eye = lax.broadcasted_iota(jnp.int32, (LANE, LANE), 0) == lax.broadcasted_iota(jnp.int32, (LANE, LANE), 1)

    def run(tails, wire):
        def body(r, carry):
            base = r * LANE
            lanes = pl.ds(pl.multiple_of(base, LANE), LANE)
            grad = []
            for j in range(CH):
                part = chunk(head_ref, j, LANE, base)
                grad.append(part + wire_get(tails, lanes, j, dim) if kinds else part)
            square = jnp.sum(sum(g * g for g in grad), axis=1, keepdims=True)
            state = jnp.sum(jnp.where(eye, state_ref[r], 0.0), axis=1, keepdims=True) + square / dim
            new_state[r] = jnp.sum(jnp.where(eye, state, 0.0), axis=0, keepdims=True)
            rate = LEARN_ENT * lax.rsqrt(state + ADA_EPS)
            for j in range(CH):
                new = chunk(ent_ref, j, LANE, base) - rate * grad[j]
                if final:
                    wire_put(new_ref, lanes, j, dim, new)
                else:
                    put_chunk(new_ref, j, LANE, new, base)
                if wire is not None:
                    wire_put(wire, lanes, j, dim, new)
            return carry
        lax.fori_loop(0, WBLK // LANE, body, 0, unroll=True)

    if not kinds and not outs:
        run(None, None)
        return
    for p in range(PIECES):
        now = at // per == p
        wire = wires[p] if outs else None
        if not kinds:
            pl.when(now)(functools.partial(run, None, wire))
        if "first" in kinds:
            pl.when(now)(functools.partial(run, parts["first"][p], wire))
        if "second" in kinds:
            pl.when(now & (near == 0))(functools.partial(run, parts["second"][p], wire))
        if "direct" in kinds:
            pl.when(now & (near == 1))(functools.partial(run, parts["direct"][p], wire))


def update_call(flags, ent, state, head, tails, dim, late, outs, final, done=None):
    rows = ent.shape[0] // CH
    blocks = rows // WBLK
    per = blocks // (2 * PIECES)

    def at(i, flags):
        return row_block(i + late * (blocks // 2), flags[0], blocks)

    packed = pl.BlockSpec((CH * WBLK, LANE), lambda i, flags: (at(i, flags), 0))
    state_spec = pl.BlockSpec((WBLK // LANE, 1, LANE), lambda i, flags: (at(i, flags), 0, 0))
    if isinstance(tails, dict):
        kinds = [kind for kind in tails if (kind != "first") == bool(late)]
        operands = [x for kind in kinds for x in tails[kind]]
        specs = wire_in_specs(kinds, dim, blocks, late * (blocks // 2))
    else:
        kinds, operands, specs = [], [], []
    first = 1 + len(operands)
    operands = operands + [ent, head, state]
    specs = specs + [packed, packed, state_spec]
    alias = {first + 2: 1}
    width = wire_rows(dim, BF16)[1]
    mode = None
    if final:
        mode = "late" if late else "own"
        new_spec = pl.BlockSpec((dim, WBLK), lambda i, flags: (0, at(i, flags)))
        new_shape = jax.ShapeDtypeStruct((dim, rows), F32)
        if late:
            operands, specs = operands + [done], specs + [pl.BlockSpec(memory_space=pl.ANY)]
            alias[first + 3] = 0
    else:
        new_spec, new_shape = packed, jax.ShapeDtypeStruct(ent.shape, F32)
        alias[first] = 0
    count = PIECES if outs else 0
    return pl.pallas_call(
        functools.partial(update_kernel, dim, blocks, kinds, outs, mode),
        grid_spec=pltpu.PrefetchScalarGridSpec(
            num_scalar_prefetch=1,
            grid=(blocks // 2,),
            in_specs=specs,
            out_specs=[new_spec, state_spec] + [
                pl.BlockSpec((width, WBLK), lambda i, *_, p=p: (0, clip_piece(i, p, per))) for p in range(count)],
        ),
        out_shape=[new_shape, jax.ShapeDtypeStruct(state.shape, F32)]
        + [jax.ShapeDtypeStruct((width, per * WBLK), BF16)] * count,
        input_output_aliases=alias,
        compiler_params=params(), cost_estimate=cost(rows * 2000, rows * 4500), name="update",
    )(flags, *operands)


def adagrad(param, state, grad, dim, rate):
    shape = (-1, CH, LANE)
    param, grad = param.reshape(shape), grad.reshape(shape)
    state = state + jnp.sum(grad * grad, axis=(1, 2)) / dim
    return (param - rate * grad * lax.rsqrt(state + ADA_EPS)[:, None, None]).reshape(-1, LANE), state


def solution(mesh):
    ent_size = mesh.shape["ent"]
    data_size = mesh.shape["data"]
    axes = ("data", "ent")

    def dev(j, i):
        return j * ent_size + i

    def split(pairs):
        return [(i, k) for i, k in pairs if i // 2 != k // 2], [(i, k) for i, k in pairs if i // 2 == k // 2]

    rows = range(data_size)

    def send_own(own, pairs):
        return [lax.ppermute(x, axes, [(dev(j, i), dev(j, k)) for j in rows for i, k in pairs]) for x in own]

    def send_other(other, pairs):
        near = split(pairs)[1]
        return [lax.ppermute(x, axes, [(dev(j, i), dev(j, k)) for j in rows for i, k in near]) for x in other]

    def swap(first, pairs):
        cross = split(pairs)[0]
        return [lax.ppermute(x, axes, [(dev(j, k), dev(1 - j, k)) for j in rows for _, k in cross]) for x in first]

    def device_epoch(ent_table, ada_state, rel_table, head_idx, tail_idx, rel_idx, edge_mask, neg_idx):
        dim_rows, dim = ent_table.shape
        edge_count = head_idx.shape[-1]
        idle, *ids = lax.sort(
            (1 - edge_mask[0, 0], head_idx[0, 0], tail_idx[0, 0], rel_idx[0, 0]), dimension=1, num_keys=1, is_stable=False)
        live = jnp.broadcast_to(jnp.sum(1 - idle, axis=1, keepdims=True), (ent_size, LANE))
        ids = [mark_groups(x, size) for x, size in zip(ids, (GROUP, GROUP, REL_GROUP))]
        packed = lax.all_gather(jnp.concatenate(ids + [neg_idx[0, 0] * CH, live], axis=1), "data")
        ent = pack_call(ent_table.T)
        state = ada_state.reshape(-1, 1, LANE)
        rel = pack_rows(rel_table)
        rel_state = jnp.zeros((rel_table.shape[0],), F32)
        mine, me = lax.axis_index("data"), lax.axis_index("ent")
        losses = []
        tails = ent
        fetch = [(i, i) for i in range(ent_size)]
        for s in range(ent_size):
            now = packed[:, s]
            hid, tid, rid = (now[:, i * edge_count:(i + 1) * edge_count].reshape(-1) for i in range(3))
            nid = now[:, 3 * edge_count:-LANE].reshape(-1)
            cnt = now[:, -1]
            back = [(k, i) for i, k in fetch]
            back_near = s > 0 and bool(split(back)[1])
            final = s == ent_size - 1
            nxt = [((i + s + 1) % ent_size, i) for i in range(ent_size)]
            nxt_near = bool(split(nxt)[1])

            def flags_of(pairs):
                near = [k for _, k in split(pairs)[1]]
                hit = functools.reduce(jnp.logical_or, [me == k for k in near], jnp.bool_(False))
                return jnp.stack([mine, hit.astype(jnp.int32)]).astype(jnp.int32)

            fetch_flags, back_flags = flags_of(fetch), flags_of(back)
            q, a = query_call(cnt, hid, rid, ent, rel)
            dq, tg, neg, loss = main_call(fetch_flags, cnt, tid, nid, tails, q, dim_rows, dim)
            tail_grad, local = None, (tid, nid, tg, neg)
            if s:
                pieces = tail_call(fetch_flags, cnt, *local, dim_rows, dim, back_near)
                tail_grad, local = {"first": send_own(pieces[:PIECES], back)}, None
                if back_near:
                    tail_grad["direct"] = send_other(pieces[PIECES:], back)
            head_grad, rel_grad = head_call(cnt, hid, rid, rel, dq, a, dim_rows, local)
            rel_grad = lax.psum(rel_grad, "ent")
            if s:
                ready = []
                for x in tail_grad["first"]:
                    x, head_grad = lax.optimization_barrier((x, head_grad))
                    ready.append(x)
                tail_grad["first"] = ready
                tail_grad["second"] = swap(ready, back)
            new_ent, state, *own = update_call(
                back_flags, ent, state, head_grad, tail_grad, dim, 0, not final, final)
            if not final:
                own, rel_grad = lax.optimization_barrier((own, rel_grad))
                tails = {"first": send_own(own, nxt)}
                ent, state, *other = update_call(
                    back_flags, new_ent, state, head_grad, tail_grad, dim, 1, nxt_near, False)
                ready = []
                for x in tails["first"]:
                    x, ent = lax.optimization_barrier((x, ent))
                    ready.append(x)
                tails["first"] = ready
                tails["second"] = swap(ready, nxt)
                if nxt_near:
                    tails["direct"] = send_other(other, nxt)
            else:
                new_ent, rel_grad = lax.optimization_barrier((new_ent, rel_grad))
                ent, state = update_call(
                    back_flags, ent, state, head_grad, tail_grad, dim, 1, False, True, new_ent)
            rel, rel_state = adagrad(rel, rel_state, rel_grad, dim, LEARN_REL)
            losses.append(jnp.where(mine == 0, loss[0, 0, 0], loss[1, 0, 0]) / edge_count)
            fetch = nxt
        return ent.T, state.reshape(-1), unpack_rows(rel, dim), jnp.stack(losses)[None, None, :]

    ent_spec = P(("sweep", "ent"), None)
    row_spec = P(("sweep", "ent"))
    rel_spec = P("sweep", None)
    edge_spec = P(("sweep", "ent"), "data", None, None)
    loss_spec = P(("sweep", "ent"), "data", None)
    return jax.shard_map(
        device_epoch, mesh=mesh,
        in_specs=(ent_spec, row_spec, rel_spec, edge_spec, edge_spec, edge_spec, edge_spec, edge_spec),
        out_specs=(ent_spec, row_spec, rel_spec, loss_spec),
        check_vma=False)
```

```python
import functools

import jax
import jax.numpy as jnp
from jax import lax
from jax.experimental import pallas as pl
from jax.experimental.pallas import tpu as pltpu
from jax.sharding import PartitionSpec as P


LEARN_ENT = 0.1
LEARN_REL = 0.05
ADA_EPS = 1e-6

CH = 4
LANE = 128
BLK = 512
GROUP = 16
REL_GROUP = 8
UNROLL = 8
WBLK = 1024
PIECES = 2
VMEM_LIMIT = 64 * 1024 * 1024 - 65536
F32 = jnp.float32
BF16 = jnp.bfloat16


def params():
    return pltpu.CompilerParams(dimension_semantics=("arbitrary",), vmem_limit_bytes=VMEM_LIMIT)


def cost(flops, bytes_accessed):
    return pl.CostEstimate(flops=flops, bytes_accessed=bytes_accessed, transcendentals=0)


def row_at(n):
    return pl.ds(pl.multiple_of(n * CH, CH), CH)


def id_row(ids, at, leads, off=0):
    value = ids.at[pl.ds(at, off + 1)][off]
    return pl.ds(pl.multiple_of(value & -CH if leads else value, CH), CH)


def mark_groups(ids, size):
    count = ids.shape[-1]
    place = lax.broadcasted_iota(jnp.int32, ids.shape, ids.ndim - 1) % size
    hit = jnp.zeros(ids.shape, jnp.int32)
    for k in range(1, size):
        hit = hit | ((ids == jnp.roll(ids, k, axis=-1)) & (place >= k)).astype(jnp.int32)
    k = 1
    while k < size:
        hit = hit | jnp.roll(hit, -k, axis=-1)
        k *= 2
    return ids * CH + jnp.where(place == 0, hit, 0)


def chunk(buf, j, count, base=0):
    return buf[pl.ds(base * CH + j, count, stride=CH), :]


def put_chunk(buf, j, count, val, base=0):
    buf[pl.ds(base * CH + j, count, stride=CH), :] = val


def pack_rows(x):
    rows, dim = x.shape
    half = dim // 2
    x = jnp.pad(x.reshape(rows, 2, half), ((0, 0), (0, 0), (0, 2 * LANE - half)))
    return x.reshape(rows * CH, LANE)


def unpack_rows(x, dim):
    rows = x.shape[0] // CH
    return x.reshape(rows, 2, 2 * LANE)[:, :, :dim // 2].reshape(rows, dim)


def columns_t(x, size):
    return x if size == LANE else jnp.concatenate([x, jnp.zeros((LANE - size, LANE), F32)], axis=0)


def wire_get(ref, lanes, dim):
    half = dim // 2
    rest = half - LANE
    if ref.dtype == F32:
        parts = [ref[pl.ds(off, size), lanes] for off, size in ((0, LANE), (LANE, rest), (half, LANE), (half + LANE, rest))]
    else:
        tail = ref[pl.ds(2 * LANE, 2 * rest), lanes].astype(F32)
        parts = [ref[pl.ds(0, LANE), lanes].astype(F32), tail[:rest], ref[pl.ds(LANE, LANE), lanes].astype(F32), tail[rest:]]
    return [columns_t(x, x.shape[0]).T for x in parts]


def wire_put(ref, lanes, dim, vals):
    half = dim // 2
    rest = half - LANE
    t = [v.T for v in vals]
    if ref.dtype == F32:
        for x, off, size in zip(t, (0, LANE, half, half + LANE), (LANE, rest, LANE, rest)):
            ref[pl.ds(off, size), lanes] = x[:size]
    else:
        ref[pl.ds(0, LANE), lanes] = t[0].astype(BF16)
        ref[pl.ds(LANE, LANE), lanes] = t[2].astype(BF16)
        ref[pl.ds(2 * LANE, 2 * rest), lanes] = jnp.concatenate([t[1][:rest], t[3][:rest]], axis=0).astype(BF16)


def clip_piece(t, p, per):
    return jnp.clip(t - p * per, 0, per - 1)


def row_block(t, mine, blocks):
    half = blocks // 2
    return jnp.where(t < half, mine * half + t, (1 - mine) * half + t - half)


def gather_rows(ids, base, table, buf, count):
    def body(t, carry):
        e = t * UNROLL
        for u in range(UNROLL):
            buf[row_at(e + u), :] = table[id_row(ids, base + e, u == 0, u), :]
        return carry
    lax.fori_loop(0, count // UNROLL, body, 0)


def group_rows(ids, at, size, lead):
    return [id_row(ids, at, g % lead == 0, g) for g in range(size)]


def add_one(row, e, buf, acc):
    acc[row, :] += buf[row_at(e), :]


def add_group(at, e, buf, acc):
    total = [acc[row, :] + buf[row_at(e + g), :] for g, row in enumerate(at)]
    for row, value in zip(at, total):
        acc[row, :] = value


def scatter_rows(ids, base, buf, acc, count):
    def body(t, carry):
        e = t * GROUP

        def fast():
            add_group(group_rows(ids, base + e, GROUP, GROUP), e, buf, acc)

        def slow():
            for g, row in enumerate(group_rows(ids, base + e, GROUP, GROUP)):
                add_one(row, e + g, buf, acc)

        lax.cond((ids[base + e] & 1) == 0, fast, slow)
        return carry
    lax.fori_loop(0, count // GROUP, body, 0)


def scatter_plain(ids, buf, acc, count):
    def body(t, carry):
        e = t * UNROLL
        for u, row in enumerate(group_rows(ids, e, UNROLL, UNROLL)):
            add_one(row, e + u, buf, acc)
        return carry
    lax.fori_loop(0, count // UNROLL, body, 0)


def zero_rows(acc):
    rows = acc.shape[0]
    size = 512

    def body(t, carry):
        acc[pl.ds(pl.multiple_of(t * size, size), size), :] = jnp.zeros((size, LANE), F32)
        return carry
    full = rows // size
    lax.fori_loop(0, full, body, 0)
    if rows % size:
        acc[full * size:, :] = jnp.zeros((rows % size, LANE), F32)


def block_live(step, steps, cnt):
    return (step % steps) * BLK < cnt[step // steps]


def edge_block(i, steps, cnt):
    shard = i // steps
    last = jnp.maximum((cnt[shard] + (BLK - 1)) // BLK - 1, 0)
    return shard * steps + jnp.minimum(i % steps, last)


def run_copy(src, dst, sem):
    copy = pltpu.make_async_copy(src, dst, sem)
    copy.start()
    copy.wait()


def pack_kernel(dim, x_ref, out_ref):
    for r in range(WBLK // LANE):
        for j, x in enumerate(wire_get(x_ref, pl.ds(r * LANE, LANE), dim)):
            put_chunk(out_ref, j, LANE, x, r * LANE)


def pack_call(x):
    dim, rows = x.shape
    return pl.pallas_call(
        functools.partial(pack_kernel, dim),
        grid=(rows // WBLK,),
        in_specs=[pl.BlockSpec((dim, WBLK), lambda i: (0, i))],
        out_specs=pl.BlockSpec((CH * WBLK, LANE), lambda i: (i, 0)),
        out_shape=jax.ShapeDtypeStruct((CH * rows, LANE), F32),
        compiler_params=params(), cost_estimate=cost(rows, rows * 4096), name="pack",
    )(x)


def query_kernel(steps, cnt, hid, rid, ent_hbm, rel_ref, q_ref, a_ref, r_ref, ent, abuf, rbuf, sem):
    step = pl.program_id(0)

    @pl.when(step == 0)
    def _():
        run_copy(ent_hbm, ent, sem)

    @pl.when(block_live(step, steps, cnt))
    def _():
        base = step * BLK

        def body(t, carry):
            e = t * UNROLL
            for u in range(UNROLL):
                abuf[row_at(e + u), :] = ent[id_row(hid, base + e, u == 0, u), :]
                rbuf[row_at(e + u), :] = rel_ref[id_row(rid, base + e, u == 0, u), :]
            return carry
        lax.fori_loop(0, BLK // UNROLL, body, 0)
        for j in range(2):
            a_re, a_im = chunk(abuf, j, BLK), chunk(abuf, j + 2, BLK)
            r_re, r_im = chunk(rbuf, j, BLK), chunk(rbuf, j + 2, BLK)
            q_ref[j] = a_re * r_re - a_im * r_im
            q_ref[j + 2] = a_re * r_im + a_im * r_re
            a_ref[j] = a_re
            a_ref[j + 2] = a_im
            r_ref[j] = r_re
            r_ref[j + 2] = r_im


def query_call(cnt, hid, rid, ent, rel):
    edges = hid.shape[0]
    steps = edges // cnt.shape[0] // BLK
    edge_spec = pl.BlockSpec((CH, BLK, LANE), lambda i, cnt, *_: (0, edge_block(i, steps, cnt), 0))
    return pl.pallas_call(
        functools.partial(query_kernel, steps),
        grid_spec=pltpu.PrefetchScalarGridSpec(
            num_scalar_prefetch=3,
            grid=(edges // BLK,),
            in_specs=[
                pl.BlockSpec(memory_space=pl.ANY),
                pl.BlockSpec(rel.shape, lambda i, *_: (0, 0)),
            ],
            out_specs=[edge_spec] * 3,
            scratch_shapes=[
                pltpu.VMEM(ent.shape, F32),
                pltpu.VMEM((BLK * CH, LANE), F32),
                pltpu.VMEM((BLK * CH, LANE), F32),
                pltpu.SemaphoreType.DMA,
            ],
        ),
        out_shape=[jax.ShapeDtypeStruct((CH, edges, LANE), F32)] * 3,
        compiler_params=params(), cost_estimate=cost(edges * 3000, edges * 6144), name="query",
    )(cnt, hid, rid, ent, rel)


def main_kernel(steps, loads, wired, kinds, dim, flags, cnt, tid, nid, *refs):
    parts = {}
    refs = list(refs)
    if wired:
        for kind in kinds:
            parts[kind] = [refs.pop(0) for _ in range(PIECES)]
    else:
        ent_hbm = refs.pop(0)
    q_ref, dq_ref, tg_ref, neg_ref, loss_ref, ent, cbuf, mbuf, nacc = refs[:9]
    at = pl.program_id(0)
    negs = mbuf.shape[0]

    if wired:
        per = loads // (2 * PIECES)
        mine, near = flags[0], flags[1]

        def fill(ref):
            base = row_block(at, mine, loads) * WBLK

            def body(r, carry):
                lanes = pl.ds(pl.multiple_of(r * LANE, LANE), LANE)
                for j, x in enumerate(wire_get(ref, lanes, dim)):
                    put_chunk(ent, j, LANE, x, base + r * LANE)
                return carry
            lax.fori_loop(0, WBLK // LANE, body, 0, unroll=True)

        for p in range(PIECES):
            pl.when(at // per == p)(functools.partial(fill, parts["first"][p]))
            late = at // per == PIECES + p
            if "second" in kinds:
                pl.when(late & (near == 0))(functools.partial(fill, parts["second"][p]))
            if "direct" in kinds:
                pl.when(late & (near == 1))(functools.partial(fill, parts["direct"][p]))
    else:
        @pl.when(at == 0)
        def _():
            run_copy(ent_hbm, ent, refs[9])

    step = jnp.maximum(at - loads, 0)
    shard = step // steps
    live = at >= loads

    @pl.when(live & (step % steps == 0))
    def _():
        for start in range(0, negs, min(BLK, negs)):
            gather_rows(nid, shard * negs + start, ent, cbuf, min(BLK, negs))
            for j in range(CH):
                mbuf[pl.ds(start, min(BLK, negs)), pl.ds(j * LANE, LANE)] = chunk(cbuf, j, min(BLK, negs)).astype(BF16)
        nacc[...] = jnp.zeros_like(nacc)
        loss_ref[...] = jnp.zeros_like(loss_ref)

    @pl.when(live & block_live(step, steps, cnt))
    def _():
        gather_rows(tid, step * BLK, ent, cbuf, BLK)
        c = [chunk(cbuf, j, BLK).astype(BF16).astype(F32) for j in range(CH)]
        q = [q_ref[j] for j in range(CH)]
        p = jnp.sum(q[0] * c[0] + q[1] * c[1] + q[2] * c[2] + q[3] * c[3], axis=1, keepdims=True)
        q_bf = jnp.concatenate([x.astype(BF16) for x in q], axis=1)
        m = mbuf[...]
        s = lax.dot_general(q_bf, m, (((1,), (1,)), ((), ())), preferred_element_type=F32)
        place = lax.broadcasted_iota(jnp.int32, (BLK, 1), 0) + (step % steps) * BLK
        w = jnp.where(place < cnt[shard], 1.0, 0.0)
        top = jnp.maximum(p, jnp.max(s, axis=1, keepdims=True))
        p_exp = jnp.exp(p - top)
        n_exp = jnp.exp(s - top)
        norm = p_exp + jnp.sum(n_exp, axis=1, keepdims=True)
        loss = jnp.sum(w * (top + jnp.log(norm) - p), axis=0, keepdims=True)
        loss_ref[...] += jnp.broadcast_to(loss[None], loss_ref.shape)
        alpha = w * (p_exp / norm - 1.0)
        beta = ((w / norm) * n_exp).astype(BF16)
        back = jnp.dot(beta, m, preferred_element_type=F32)
        for j in range(CH):
            dq_ref[j] = alpha * c[j] + back[:, j * LANE:(j + 1) * LANE]
            put_chunk(tg_ref, j, BLK, alpha * q[j])
        nacc[...] += lax.dot_general(beta, q_bf, (((0,), (0,)), ((), ())), preferred_element_type=F32)

    @pl.when(live & (step % steps == steps - 1))
    def _():
        for j in range(CH):
            put_chunk(neg_ref, j, negs, nacc[:, j * LANE:(j + 1) * LANE])


def wire_in_specs(kinds, width, blocks, shift=0):
    per = blocks // (2 * PIECES)
    specs = []
    for kind in kinds:
        for p in range(PIECES):
            def index(i, flags, *_, kind=kind, p=p):
                if kind == "first":
                    return 0, clip_piece(i + shift, p, per)
                used = flags[1] if kind == "direct" else 1 - flags[1]
                return 0, clip_piece(i + shift, PIECES + p, per) * used
            specs.append(pl.BlockSpec((width, WBLK), index))
    return specs


def main_call(flags, cnt, tid, nid, tails, q, rows, dim):
    edges = tid.shape[0]
    shards = cnt.shape[0]
    negs = nid.shape[0] // shards
    steps = edges // shards // BLK
    wired = isinstance(tails, dict)
    if wired:
        loads, kinds = rows // WBLK, list(tails)
        operands = [x for kind in kinds for x in tails[kind]]
        specs = wire_in_specs(kinds, operands[0].shape[0], loads)
        sems = []
    else:
        loads, kinds, operands, specs = 0, [], [tails], [pl.BlockSpec(memory_space=pl.ANY)]
        sems = [pltpu.SemaphoreType.DMA]

    def block(i, cnt):
        return edge_block(jnp.maximum(i - loads, 0), steps, cnt)

    def shard_of(i):
        return jnp.maximum(i - loads, 0) // steps

    edge_spec = pl.BlockSpec((CH, BLK, LANE), lambda i, flags, cnt, *_: (0, block(i, cnt), 0))
    return pl.pallas_call(
        functools.partial(main_kernel, steps, loads, wired, kinds, dim),
        grid_spec=pltpu.PrefetchScalarGridSpec(
            num_scalar_prefetch=4,
            grid=(loads + edges // BLK,),
            in_specs=specs + [edge_spec],
            out_specs=[
                edge_spec,
                pl.BlockSpec((CH * BLK, LANE), lambda i, flags, cnt, *_: (block(i, cnt), 0)),
                pl.BlockSpec((CH * negs, LANE), lambda i, *_: (shard_of(i), 0)),
                pl.BlockSpec((1, 8, LANE), lambda i, *_: (shard_of(i), 0, 0)),
            ],
            scratch_shapes=[
                pltpu.VMEM((CH * rows, LANE), F32),
                pltpu.VMEM((BLK * CH, LANE), F32),
                pltpu.VMEM((negs, CH * LANE), BF16),
                pltpu.VMEM((negs, CH * LANE), F32),
            ] + sems,
        ),
        out_shape=[
            jax.ShapeDtypeStruct((CH, edges, LANE), F32),
            jax.ShapeDtypeStruct((CH * edges, LANE), F32),
            jax.ShapeDtypeStruct((CH * negs * shards, LANE), F32),
            jax.ShapeDtypeStruct((shards, 8, LANE), F32),
        ],
        compiler_params=params(), cost_estimate=cost(edges * negs * 3072, edges * 8192), name="scores",
    )(flags, cnt, tid, nid, *operands, q)


def tail_kernel(steps, total, blocks, dim, flags, cnt, tid, nid, tg_ref, neg_ref, *refs):
    step = pl.program_id(0)
    acc = refs[-1]

    @pl.when(step == 0)
    def _():
        zero_rows(acc)
        scatter_plain(nid, neg_ref, acc, nid.shape[0])

    @pl.when((step < total) & block_live(jnp.minimum(step, total - 1), steps, cnt))
    def _():
        scatter_rows(tid, step * BLK, tg_ref, acc, BLK)

    outs = refs[:-1]
    per = blocks // (2 * PIECES)
    at = step - total

    def emit(ref):
        base = row_block(at, flags[0], blocks) * WBLK

        def body(r, carry):
            lanes = pl.ds(pl.multiple_of(r * LANE, LANE), LANE)
            wire_put(ref, lanes, dim, [chunk(acc, j, LANE, base + r * LANE) for j in range(CH)])
            return carry
        lax.fori_loop(0, WBLK // LANE, body, 0, unroll=True)

    for p, ref in enumerate(outs):
        pl.when((at >= 0) & (at // per == p))(functools.partial(emit, ref))


def tail_call(flags, cnt, tid, nid, tg, neg, rows, dim, near):
    edges = tid.shape[0]
    total = edges // BLK
    steps = total // cnt.shape[0]
    blocks = rows // WBLK
    per = blocks // (2 * PIECES)
    acc = pltpu.VMEM((CH * rows, LANE), F32)
    pieces = PIECES * (2 if near else 1)
    grid = total + pieces * per
    out_specs = [
        pl.BlockSpec((dim, WBLK), lambda i, *_, p=p: (0, clip_piece(i - total, p, per))) for p in range(pieces)]
    out_shape = [jax.ShapeDtypeStruct((dim, per * WBLK), F32)] * pieces
    scratch = [acc]
    return pl.pallas_call(
        functools.partial(tail_kernel, steps, total, blocks, dim),
        grid_spec=pltpu.PrefetchScalarGridSpec(
            num_scalar_prefetch=4,
            grid=(grid,),
            in_specs=[
                pl.BlockSpec((CH * BLK, LANE),
                             lambda i, flags, cnt, *_: (edge_block(jnp.minimum(i, total - 1), steps, cnt), 0)),
                pl.BlockSpec(neg.shape, lambda i, *_: (0, 0)),
            ],
            out_specs=out_specs,
            scratch_shapes=scratch,
        ),
        out_shape=out_shape,
        compiler_params=params(), cost_estimate=cost(edges * 3000, edges * 6144), name="tails",
    )(flags, cnt, tid, nid, tg, neg)


def head_kernel(steps, both, cnt, hid, rid, *refs):
    refs = list(refs)
    if both:
        tid, nid = refs.pop(0), refs.pop(0)
        tg_ref, neg_ref = refs.pop(0), refs.pop(0)
    r_ref, dq_ref, a_ref, out_hbm, racc_hbm, acc, racc, hbuf, gbuf, sem, rsem = refs
    step = pl.program_id(0)

    @pl.when(step == 0)
    def _():
        zero_rows(acc)
        zero_rows(racc)
        if both:
            scatter_plain(nid, neg_ref, acc, nid.shape[0])

    @pl.when(block_live(step, steps, cnt))
    def _():
        base = step * BLK
        for j in range(2):
            d_re, d_im = dq_ref[j], dq_ref[j + 2]
            r_re, r_im = r_ref[j], r_ref[j + 2]
            put_chunk(hbuf, j, BLK, d_re * r_re + d_im * r_im)
            put_chunk(hbuf, j + 2, BLK, d_im * r_re - d_re * r_im)
            a_re, a_im = a_ref[j], a_ref[j + 2]
            put_chunk(gbuf, j, BLK, d_re * a_re + d_im * a_im)
            put_chunk(gbuf, j + 2, BLK, d_im * a_re - d_re * a_im)

        def body(t, carry):
            e = t * GROUP
            repeat = hid[base + e]
            for g in range(0, GROUP, REL_GROUP):
                repeat = repeat | rid[base + e + g]

            def fast():
                add_group(group_rows(hid, base + e, GROUP, GROUP), e, hbuf, acc)
                for g in range(0, GROUP, REL_GROUP):
                    add_group(group_rows(rid, base + e + g, REL_GROUP, REL_GROUP), e + g, gbuf, racc)

            def slow():
                for g in range(GROUP):
                    add_one(id_row(hid, base + e, g == 0, g), e + g, hbuf, acc)
                    add_one(id_row(rid, base + e, g % REL_GROUP == 0, g), e + g, gbuf, racc)

            lax.cond((repeat & 1) == 0, fast, slow)
            return carry
        lax.fori_loop(0, BLK // GROUP, body, 0)
        if both:
            scatter_rows(tid, base, tg_ref, acc, BLK)

    @pl.when(step == pl.num_programs(0) - 1)
    def _():
        copy = pltpu.make_async_copy(acc, out_hbm, sem)
        copy.start()
        rcopy = pltpu.make_async_copy(racc, racc_hbm, rsem)
        rcopy.start()
        copy.wait()
        rcopy.wait()


def head_call(cnt, hid, rid, r, dq, a, rows, rels, tails=None):
    edges = hid.shape[0]
    steps = edges // cnt.shape[0] // BLK
    both = tails is not None
    scalars, operands, specs = [cnt, hid, rid], [], []
    if both:
        tid, nid, tg, neg = tails
        scalars += [tid, nid]
        operands = [tg, neg]
        specs = [pl.BlockSpec((CH * BLK, LANE), lambda i, cnt, *_: (edge_block(i, steps, cnt), 0)),
                 pl.BlockSpec(neg.shape, lambda i, *_: (0, 0))]
    edge_spec = pl.BlockSpec((CH, BLK, LANE), lambda i, cnt, *_: (0, edge_block(i, steps, cnt), 0))
    return pl.pallas_call(
        functools.partial(head_kernel, steps, both),
        grid_spec=pltpu.PrefetchScalarGridSpec(
            num_scalar_prefetch=len(scalars),
            grid=(edges // BLK,),
            in_specs=specs + [edge_spec] * 3,
            out_specs=[pl.BlockSpec(memory_space=pl.ANY)] * 2,
            scratch_shapes=[
                pltpu.VMEM((CH * rows, LANE), F32),
                pltpu.VMEM((CH * rels, LANE), F32),
                pltpu.VMEM((BLK * CH, LANE), F32),
                pltpu.VMEM((BLK * CH, LANE), F32),
                pltpu.SemaphoreType.DMA,
                pltpu.SemaphoreType.DMA,
            ],
        ),
        out_shape=[jax.ShapeDtypeStruct((CH * rows, LANE), F32), jax.ShapeDtypeStruct((CH * rels, LANE), F32)],
        compiler_params=params(), cost_estimate=cost(edges * 6000, edges * 8192), name="heads",
    )(*scalars, *operands, r, dq, a)


def update_kernel(dim, blocks, kinds, outs, final, flags, *refs):
    refs = list(refs)
    parts = {kind: [refs.pop(0) for _ in range(PIECES)] for kind in kinds}
    ent_ref, head_ref, state_ref = refs[:3]
    if final == "late":
        refs.pop(3)
    new_ref, new_state = refs[3:5]
    wires = refs[5:]
    at = pl.program_id(0)
    per = blocks // (2 * PIECES)
    near = flags[1]
    eye = lax.broadcasted_iota(jnp.int32, (LANE, LANE), 0) == lax.broadcasted_iota(jnp.int32, (LANE, LANE), 1)

    def run(tails, wire):
        def body(r, carry):
            base = r * LANE
            lanes = pl.ds(pl.multiple_of(base, LANE), LANE)
            grad = [chunk(head_ref, j, LANE, base) for j in range(CH)]
            if kinds:
                grad = [x + y for x, y in zip(grad, wire_get(tails, lanes, dim))]
            square = jnp.sum(sum(g * g for g in grad), axis=1, keepdims=True)
            state = jnp.sum(jnp.where(eye, state_ref[r], 0.0), axis=1, keepdims=True) + square / dim
            new_state[r] = jnp.sum(jnp.where(eye, state, 0.0), axis=0, keepdims=True)
            rate = LEARN_ENT * lax.rsqrt(state + ADA_EPS)
            new = [chunk(ent_ref, j, LANE, base) - rate * grad[j] for j in range(CH)]
            if final:
                wire_put(new_ref, lanes, dim, new)
            else:
                for j in range(CH):
                    put_chunk(new_ref, j, LANE, new[j], base)
            if wire is not None:
                wire_put(wire, lanes, dim, new)
            return carry
        lax.fori_loop(0, WBLK // LANE, body, 0, unroll=True)

    if not kinds and not outs:
        run(None, None)
        return
    for p in range(PIECES):
        now = at // per == p
        wire = wires[p] if outs else None
        if not kinds:
            pl.when(now)(functools.partial(run, None, wire))
        if "first" in kinds:
            pl.when(now)(functools.partial(run, parts["first"][p], wire))
        if "second" in kinds:
            pl.when(now & (near == 0))(functools.partial(run, parts["second"][p], wire))
        if "direct" in kinds:
            pl.when(now & (near == 1))(functools.partial(run, parts["direct"][p], wire))


def update_call(flags, ent, state, head, tails, dim, late, outs, final, done=None):
    rows = ent.shape[0] // CH
    blocks = rows // WBLK
    per = blocks // (2 * PIECES)

    def at(i, flags):
        return row_block(i + late * (blocks // 2), flags[0], blocks)

    packed = pl.BlockSpec((CH * WBLK, LANE), lambda i, flags: (at(i, flags), 0))
    state_spec = pl.BlockSpec((WBLK // LANE, 1, LANE), lambda i, flags: (at(i, flags), 0, 0))
    if isinstance(tails, dict):
        kinds = [kind for kind in tails if (kind != "first") == bool(late)]
        operands = [x for kind in kinds for x in tails[kind]]
        specs = wire_in_specs(kinds, dim, blocks, late * (blocks // 2))
    else:
        kinds, operands, specs = [], [], []
    first = 1 + len(operands)
    operands = operands + [ent, head, state]
    specs = specs + [packed, packed, state_spec]
    alias = {first + 2: 1}
    mode = None
    if final:
        mode = "late" if late else "own"
        new_spec = pl.BlockSpec((dim, WBLK), lambda i, flags: (0, at(i, flags)))
        new_shape = jax.ShapeDtypeStruct((dim, rows), F32)
        if late:
            operands, specs = operands + [done], specs + [pl.BlockSpec(memory_space=pl.ANY)]
            alias[first + 3] = 0
    else:
        new_spec, new_shape = packed, jax.ShapeDtypeStruct(ent.shape, F32)
        alias[first] = 0
    count = PIECES if outs else 0
    return pl.pallas_call(
        functools.partial(update_kernel, dim, blocks, kinds, outs, mode),
        grid_spec=pltpu.PrefetchScalarGridSpec(
            num_scalar_prefetch=1,
            grid=(blocks // 2,),
            in_specs=specs,
            out_specs=[new_spec, state_spec] + [
                pl.BlockSpec((dim, WBLK), lambda i, *_, p=p: (0, clip_piece(i, p, per))) for p in range(count)],
        ),
        out_shape=[new_shape, jax.ShapeDtypeStruct(state.shape, F32)]
        + [jax.ShapeDtypeStruct((dim, per * WBLK), BF16)] * count,
        input_output_aliases=alias,
        compiler_params=params(), cost_estimate=cost(rows * 2000, rows * 4500), name="update",
    )(flags, *operands)


def adagrad(param, state, grad, dim, rate):
    shape = (-1, CH, LANE)
    param, grad = param.reshape(shape), grad.reshape(shape)
    state = state + jnp.sum(grad * grad, axis=(1, 2)) / dim
    return (param - rate * grad * lax.rsqrt(state + ADA_EPS)[:, None, None]).reshape(-1, LANE), state


def solution(mesh):
    ent_size = mesh.shape["ent"]
    data_size = mesh.shape["data"]
    axes = ("data", "ent")

    def dev(j, i):
        return j * ent_size + i

    def split(pairs):
        return [(i, k) for i, k in pairs if i // 2 != k // 2], [(i, k) for i, k in pairs if i // 2 == k // 2]

    rows = range(data_size)

    def send_own(own, pairs):
        return [lax.ppermute(x, axes, [(dev(j, i), dev(j, k)) for j in rows for i, k in pairs]) for x in own]

    def send_other(other, pairs):
        near = split(pairs)[1]
        return [lax.ppermute(x, axes, [(dev(j, i), dev(j, k)) for j in rows for i, k in near]) for x in other]

    def swap(first, pairs):
        cross = split(pairs)[0]
        return [lax.ppermute(x, axes, [(dev(j, k), dev(1 - j, k)) for j in rows for _, k in cross]) for x in first]

    def device_epoch(ent_table, ada_state, rel_table, head_idx, tail_idx, rel_idx, edge_mask, neg_idx):
        dim_rows, dim = ent_table.shape
        edge_count = head_idx.shape[-1]
        idle, *ids = lax.sort(
            (1 - edge_mask[0, 0], head_idx[0, 0], tail_idx[0, 0], rel_idx[0, 0]), dimension=1, num_keys=1, is_stable=False)
        live = jnp.broadcast_to(jnp.sum(1 - idle, axis=1, keepdims=True), (ent_size, LANE))
        ids = [mark_groups(x, size) for x, size in zip(ids, (GROUP, GROUP, REL_GROUP))]
        packed = lax.all_gather(jnp.concatenate(ids + [neg_idx[0, 0] * CH, live], axis=1), "data")
        ent = pack_call(ent_table.T)
        state = ada_state.reshape(-1, 1, LANE)
        rel = pack_rows(rel_table)
        rel_state = jnp.zeros((rel_table.shape[0],), F32)
        mine, me = lax.axis_index("data"), lax.axis_index("ent")
        losses = []
        tails = ent
        fetch = [(i, i) for i in range(ent_size)]
        for s in range(ent_size):
            now = packed[:, s]
            hid, tid, rid = (now[:, i * edge_count:(i + 1) * edge_count].reshape(-1) for i in range(3))
            nid = now[:, 3 * edge_count:-LANE].reshape(-1)
            cnt = now[:, -1]
            back = [(k, i) for i, k in fetch]
            back_near = s > 0 and bool(split(back)[1])
            final = s == ent_size - 1
            nxt = [((i + s + 1) % ent_size, i) for i in range(ent_size)]
            nxt_near = bool(split(nxt)[1])

            def flags_of(pairs):
                near = [k for _, k in split(pairs)[1]]
                hit = functools.reduce(jnp.logical_or, [me == k for k in near], jnp.bool_(False))
                return jnp.stack([mine, hit.astype(jnp.int32)]).astype(jnp.int32)

            fetch_flags, back_flags = flags_of(fetch), flags_of(back)
            q, a, r = query_call(cnt, hid, rid, ent, rel)
            if s and "second" not in tails:
                rest = [lax.optimization_barrier((x, q))[0] for x in tails["first"][1:]]
                tails["first"] = tails["first"][:1] + rest
                tails["second"] = swap(tails["first"], fetch)
            dq, tg, neg, loss = main_call(fetch_flags, cnt, tid, nid, tails, q, dim_rows, dim)
            tail_grad, local = None, (tid, nid, tg, neg)
            if s:
                pieces = tail_call(fetch_flags, cnt, *local, dim_rows, dim, back_near)
                tail_grad, local = {"first": send_own(pieces[:PIECES], back)}, None
                if back_near:
                    tail_grad["direct"] = send_other(pieces[PIECES:], back)
            head_grad, rel_grad = head_call(cnt, hid, rid, r, dq, a, dim_rows, rel_table.shape[0], local)
            rel_grad = lax.psum(rel_grad, "ent")
            if s:
                ready = []
                for x in tail_grad["first"]:
                    x, head_grad = lax.optimization_barrier((x, head_grad))
                    ready.append(x)
                tail_grad["first"] = ready
                tail_grad["second"] = swap(ready, back)
            new_ent, state, *own = update_call(
                back_flags, ent, state, head_grad, tail_grad, dim, 0, not final, final)
            if not final:
                own, rel_grad = lax.optimization_barrier((own, rel_grad))
                tails = {"first": send_own(own, nxt)}
                ent, state, *other = update_call(
                    back_flags, new_ent, state, head_grad, tail_grad, dim, 1, nxt_near, False)
                early = s + 2 < ent_size
                if early:
                    lead, ent = lax.optimization_barrier((tails["first"][0], ent))
                    tails["first"][0] = lead
                else:
                    tails["first"] = [lax.optimization_barrier((x, state))[0] for x in tails["first"]]
                    tails["second"] = swap(tails["first"], nxt)
                if nxt_near:
                    tails["direct"] = send_other(other, nxt)
            else:
                new_ent, rel_grad = lax.optimization_barrier((new_ent, rel_grad))
                ent, state = update_call(
                    back_flags, ent, state, head_grad, tail_grad, dim, 1, False, True, new_ent)
            rel, rel_state = adagrad(rel, rel_state, rel_grad, dim, LEARN_REL)
            losses.append(jnp.where(mine == 0, loss[0, 0, 0], loss[1, 0, 0]) / edge_count)
            fetch = nxt
        return ent.T, state.reshape(-1), unpack_rows(rel, dim), jnp.stack(losses)[None, None, :]

    ent_spec = P(("sweep", "ent"), None)
    row_spec = P(("sweep", "ent"))
    rel_spec = P("sweep", None)
    edge_spec = P(("sweep", "ent"), "data", None, None)
    loss_spec = P(("sweep", "ent"), "data", None)
    return jax.shard_map(
        device_epoch, mesh=mesh,
        in_specs=(ent_spec, row_spec, rel_spec, edge_spec, edge_spec, edge_spec, edge_spec, edge_spec),
        out_specs=(ent_spec, row_spec, rel_spec, loss_spec),
        check_vma=False)
```

```python
import functools

import jax
import jax.numpy as jnp
from jax import lax
from jax.experimental import pallas as pl
from jax.experimental.pallas import tpu as pltpu
from jax.sharding import PartitionSpec as P


LEARN_ENT = 0.1
LEARN_REL = 0.05
ADA_EPS = 1e-6

CH = 4
LANE = 128
BLK = 512
GROUP = 16
REL_GROUP = 8
UNROLL = 8
WBLK = 1024
PIECES = 2
FINE = 4
VMEM_LIMIT = 64 * 1024 * 1024 - 65536
F32 = jnp.float32
BF16 = jnp.bfloat16


def params():
    return pltpu.CompilerParams(dimension_semantics=("arbitrary",), vmem_limit_bytes=VMEM_LIMIT)


def cost(flops, bytes_accessed):
    return pl.CostEstimate(flops=flops, bytes_accessed=bytes_accessed, transcendentals=0)


def row_at(n):
    return pl.ds(pl.multiple_of(n * CH, CH), CH)


def id_row(ids, at, leads, off=0):
    value = ids.at[pl.ds(at, off + 1)][off]
    return pl.ds(pl.multiple_of(value & -CH if leads else value, CH), CH)


def mark_groups(ids, size):
    count = ids.shape[-1]
    place = lax.broadcasted_iota(jnp.int32, ids.shape, ids.ndim - 1) % size
    hit = jnp.zeros(ids.shape, jnp.int32)
    for k in range(1, size):
        hit = hit | ((ids == jnp.roll(ids, k, axis=-1)) & (place >= k)).astype(jnp.int32)
    k = 1
    while k < size:
        hit = hit | jnp.roll(hit, -k, axis=-1)
        k *= 2
    return ids * CH + jnp.where(place == 0, hit, 0)


def chunk(buf, j, count, base=0):
    return buf[pl.ds(base * CH + j, count, stride=CH), :]


def put_chunk(buf, j, count, val, base=0):
    buf[pl.ds(base * CH + j, count, stride=CH), :] = val


def pack_rows(x):
    rows, dim = x.shape
    half = dim // 2
    x = jnp.pad(x.reshape(rows, 2, half), ((0, 0), (0, 0), (0, 2 * LANE - half)))
    return x.reshape(rows * CH, LANE)


def unpack_rows(x, dim):
    rows = x.shape[0] // CH
    return x.reshape(rows, 2, 2 * LANE)[:, :, :dim // 2].reshape(rows, dim)


def columns_t(x, size):
    return x if size == LANE else jnp.concatenate([x, jnp.zeros((LANE - size, LANE), F32)], axis=0)


def wire_get(ref, lanes, dim):
    half = dim // 2
    rest = half - LANE
    if ref.dtype == F32:
        parts = [ref[pl.ds(off, size), lanes] for off, size in ((0, LANE), (LANE, rest), (half, LANE), (half + LANE, rest))]
    else:
        tail = ref[pl.ds(2 * LANE, 2 * rest), lanes].astype(F32)
        parts = [ref[pl.ds(0, LANE), lanes].astype(F32), tail[:rest], ref[pl.ds(LANE, LANE), lanes].astype(F32), tail[rest:]]
    return [columns_t(x, x.shape[0]).T for x in parts]


def wire_put(ref, lanes, dim, vals):
    half = dim // 2
    rest = half - LANE
    t = [v.T for v in vals]
    if ref.dtype == F32:
        for x, off, size in zip(t, (0, LANE, half, half + LANE), (LANE, rest, LANE, rest)):
            ref[pl.ds(off, size), lanes] = x[:size]
    else:
        ref[pl.ds(0, LANE), lanes] = t[0].astype(BF16)
        ref[pl.ds(LANE, LANE), lanes] = t[2].astype(BF16)
        ref[pl.ds(2 * LANE, 2 * rest), lanes] = jnp.concatenate([t[1][:rest], t[3][:rest]], axis=0).astype(BF16)


def clip_piece(t, p, per):
    return jnp.clip(t - p * per, 0, per - 1)


def row_block(t, mine, blocks):
    half = blocks // 2
    return jnp.where(t < half, mine * half + t, (1 - mine) * half + t - half)


def gather_rows(ids, base, table, buf, count):
    def body(t, carry):
        e = t * UNROLL
        for u in range(UNROLL):
            buf[row_at(e + u), :] = table[id_row(ids, base + e, u == 0, u), :]
        return carry
    lax.fori_loop(0, count // UNROLL, body, 0)


def group_rows(ids, at, size, lead):
    return [id_row(ids, at, g % lead == 0, g) for g in range(size)]


def add_one(row, e, buf, acc):
    acc[row, :] += buf[row_at(e), :]


def add_group(at, e, buf, acc):
    total = [acc[row, :] + buf[row_at(e + g), :] for g, row in enumerate(at)]
    for row, value in zip(at, total):
        acc[row, :] = value


def scatter_rows(ids, base, buf, acc, count):
    def body(t, carry):
        e = t * GROUP

        def fast():
            add_group(group_rows(ids, base + e, GROUP, GROUP), e, buf, acc)

        def slow():
            for g, row in enumerate(group_rows(ids, base + e, GROUP, GROUP)):
                add_one(row, e + g, buf, acc)

        lax.cond((ids[base + e] & 1) == 0, fast, slow)
        return carry
    lax.fori_loop(0, count // GROUP, body, 0)


def scatter_plain(ids, buf, acc, count):
    def body(t, carry):
        e = t * UNROLL
        for u, row in enumerate(group_rows(ids, e, UNROLL, UNROLL)):
            add_one(row, e + u, buf, acc)
        return carry
    lax.fori_loop(0, count // UNROLL, body, 0)


def zero_rows(acc):
    rows = acc.shape[0]
    size = 512

    def body(t, carry):
        acc[pl.ds(pl.multiple_of(t * size, size), size), :] = jnp.zeros((size, LANE), F32)
        return carry
    full = rows // size
    lax.fori_loop(0, full, body, 0)
    if rows % size:
        acc[full * size:, :] = jnp.zeros((rows % size, LANE), F32)


def block_live(step, steps, cnt):
    return (step % steps) * BLK < cnt[step // steps]


def edge_block(i, steps, cnt):
    shard = i // steps
    last = jnp.maximum((cnt[shard] + (BLK - 1)) // BLK - 1, 0)
    return shard * steps + jnp.minimum(i % steps, last)


def run_copy(src, dst, sem):
    copy = pltpu.make_async_copy(src, dst, sem)
    copy.start()
    copy.wait()


def pack_kernel(dim, x_ref, out_ref):
    for r in range(WBLK // LANE):
        for j, x in enumerate(wire_get(x_ref, pl.ds(r * LANE, LANE), dim)):
            put_chunk(out_ref, j, LANE, x, r * LANE)


def pack_call(x):
    dim, rows = x.shape
    return pl.pallas_call(
        functools.partial(pack_kernel, dim),
        grid=(rows // WBLK,),
        in_specs=[pl.BlockSpec((dim, WBLK), lambda i: (0, i))],
        out_specs=pl.BlockSpec((CH * WBLK, LANE), lambda i: (i, 0)),
        out_shape=jax.ShapeDtypeStruct((CH * rows, LANE), F32),
        compiler_params=params(), cost_estimate=cost(rows, rows * 4096), name="pack",
    )(x)


def query_kernel(steps, cnt, hid, rid, ent_hbm, rel_ref, q_ref, a_ref, r_ref, ent, abuf, rbuf, sem):
    step = pl.program_id(0)

    @pl.when(step == 0)
    def _():
        run_copy(ent_hbm, ent, sem)

    @pl.when(block_live(step, steps, cnt))
    def _():
        base = step * BLK

        def body(t, carry):
            e = t * UNROLL
            for u in range(UNROLL):
                abuf[row_at(e + u), :] = ent[id_row(hid, base + e, u == 0, u), :]
                rbuf[row_at(e + u), :] = rel_ref[id_row(rid, base + e, u == 0, u), :]
            return carry
        lax.fori_loop(0, BLK // UNROLL, body, 0)
        for j in range(2):
            a_re, a_im = chunk(abuf, j, BLK), chunk(abuf, j + 2, BLK)
            r_re, r_im = chunk(rbuf, j, BLK), chunk(rbuf, j + 2, BLK)
            q_ref[j] = a_re * r_re - a_im * r_im
            q_ref[j + 2] = a_re * r_im + a_im * r_re
            a_ref[j] = a_re
            a_ref[j + 2] = a_im
            r_ref[j] = r_re
            r_ref[j + 2] = r_im


def query_call(cnt, hid, rid, ent, rel):
    edges = hid.shape[0]
    steps = edges // cnt.shape[0] // BLK
    edge_spec = pl.BlockSpec((CH, BLK, LANE), lambda i, cnt, *_: (0, edge_block(i, steps, cnt), 0))
    return pl.pallas_call(
        functools.partial(query_kernel, steps),
        grid_spec=pltpu.PrefetchScalarGridSpec(
            num_scalar_prefetch=3,
            grid=(edges // BLK,),
            in_specs=[
                pl.BlockSpec(memory_space=pl.ANY),
                pl.BlockSpec(rel.shape, lambda i, *_: (0, 0)),
            ],
            out_specs=[edge_spec] * 3,
            scratch_shapes=[
                pltpu.VMEM(ent.shape, F32),
                pltpu.VMEM((BLK * CH, LANE), F32),
                pltpu.VMEM((BLK * CH, LANE), F32),
                pltpu.SemaphoreType.DMA,
            ],
        ),
        out_shape=[jax.ShapeDtypeStruct((CH, edges, LANE), F32)] * 3,
        compiler_params=params(), cost_estimate=cost(edges * 3000, edges * 6144), name="query",
    )(cnt, hid, rid, ent, rel)


def main_kernel(steps, loads, wired, kinds, dim, flags, cnt, tid, nid, *refs):
    parts = {}
    refs = list(refs)
    if wired:
        for kind in kinds:
            parts[kind] = [refs.pop(0) for _ in range(PIECES)]
    else:
        ent_hbm = refs.pop(0)
    q_ref, dq_ref, tg_ref, neg_ref, loss_ref, ent, cbuf, mbuf, nacc = refs[:9]
    at = pl.program_id(0)
    negs = mbuf.shape[0]

    if wired:
        per = loads // (2 * PIECES)
        mine, near = flags[0], flags[1]

        def fill(ref):
            base = row_block(at, mine, loads) * WBLK

            def body(r, carry):
                lanes = pl.ds(pl.multiple_of(r * LANE, LANE), LANE)
                for j, x in enumerate(wire_get(ref, lanes, dim)):
                    put_chunk(ent, j, LANE, x, base + r * LANE)
                return carry
            lax.fori_loop(0, WBLK // LANE, body, 0, unroll=True)

        for p in range(PIECES):
            pl.when(at // per == p)(functools.partial(fill, parts["first"][p]))
            late = at // per == PIECES + p
            if "second" in kinds:
                pl.when(late & (near == 0))(functools.partial(fill, parts["second"][p]))
            if "direct" in kinds:
                pl.when(late & (near == 1))(functools.partial(fill, parts["direct"][p]))
    else:
        @pl.when(at == 0)
        def _():
            run_copy(ent_hbm, ent, refs[9])

    step = jnp.maximum(at - loads, 0)
    shard = step // steps
    live = at >= loads

    @pl.when(live & (step % steps == 0))
    def _():
        for start in range(0, negs, min(BLK, negs)):
            gather_rows(nid, shard * negs + start, ent, cbuf, min(BLK, negs))
            for j in range(CH):
                mbuf[pl.ds(start, min(BLK, negs)), pl.ds(j * LANE, LANE)] = chunk(cbuf, j, min(BLK, negs)).astype(BF16)
        nacc[...] = jnp.zeros_like(nacc)
        loss_ref[...] = jnp.zeros_like(loss_ref)

    @pl.when(live & block_live(step, steps, cnt))
    def _():
        gather_rows(tid, step * BLK, ent, cbuf, BLK)
        c = [chunk(cbuf, j, BLK).astype(BF16).astype(F32) for j in range(CH)]
        q = [q_ref[j] for j in range(CH)]
        p = jnp.sum(q[0] * c[0] + q[1] * c[1] + q[2] * c[2] + q[3] * c[3], axis=1, keepdims=True)
        q_bf = jnp.concatenate([x.astype(BF16) for x in q], axis=1)
        m = mbuf[...]
        s = lax.dot_general(q_bf, m, (((1,), (1,)), ((), ())), preferred_element_type=F32)
        place = lax.broadcasted_iota(jnp.int32, (BLK, 1), 0) + (step % steps) * BLK
        w = jnp.where(place < cnt[shard], 1.0, 0.0)
        top = jnp.maximum(p, jnp.max(s, axis=1, keepdims=True))
        p_exp = jnp.exp(p - top)
        n_exp = jnp.exp(s - top)
        norm = p_exp + jnp.sum(n_exp, axis=1, keepdims=True)
        loss = jnp.sum(w * (top + jnp.log(norm) - p), axis=0, keepdims=True)
        loss_ref[...] += jnp.broadcast_to(loss[None], loss_ref.shape)
        alpha = w * (p_exp / norm - 1.0)
        beta = ((w / norm) * n_exp).astype(BF16)
        back = jnp.dot(beta, m, preferred_element_type=F32)
        for j in range(CH):
            dq_ref[j] = alpha * c[j] + back[:, j * LANE:(j + 1) * LANE]
            put_chunk(tg_ref, j, BLK, alpha * q[j])
        nacc[...] += lax.dot_general(beta, q_bf, (((0,), (0,)), ((), ())), preferred_element_type=F32)

    @pl.when(live & (step % steps == steps - 1))
    def _():
        for j in range(CH):
            put_chunk(neg_ref, j, negs, nacc[:, j * LANE:(j + 1) * LANE])


def wire_in_specs(kinds, width, blocks, shift=0, count=PIECES):
    per = blocks // (2 * count)
    specs = []
    for kind in kinds:
        for p in range(count):
            def index(i, flags, *_, kind=kind, p=p):
                if kind == "first":
                    return 0, clip_piece(i + shift, p, per)
                used = flags[1] if kind == "direct" else 1 - flags[1]
                return 0, clip_piece(i + shift, count + p, per) * used
            specs.append(pl.BlockSpec((width, WBLK), index))
    return specs


def main_call(flags, cnt, tid, nid, tails, q, rows, dim):
    edges = tid.shape[0]
    shards = cnt.shape[0]
    negs = nid.shape[0] // shards
    steps = edges // shards // BLK
    wired = isinstance(tails, dict)
    if wired:
        loads, kinds = rows // WBLK, list(tails)
        operands = [x for kind in kinds for x in tails[kind]]
        specs = wire_in_specs(kinds, operands[0].shape[0], loads)
        sems = []
    else:
        loads, kinds, operands, specs = 0, [], [tails], [pl.BlockSpec(memory_space=pl.ANY)]
        sems = [pltpu.SemaphoreType.DMA]

    def block(i, cnt):
        return edge_block(jnp.maximum(i - loads, 0), steps, cnt)

    def shard_of(i):
        return jnp.maximum(i - loads, 0) // steps

    edge_spec = pl.BlockSpec((CH, BLK, LANE), lambda i, flags, cnt, *_: (0, block(i, cnt), 0))
    return pl.pallas_call(
        functools.partial(main_kernel, steps, loads, wired, kinds, dim),
        grid_spec=pltpu.PrefetchScalarGridSpec(
            num_scalar_prefetch=4,
            grid=(loads + edges // BLK,),
            in_specs=specs + [edge_spec],
            out_specs=[
                edge_spec,
                pl.BlockSpec((CH * BLK, LANE), lambda i, flags, cnt, *_: (block(i, cnt), 0)),
                pl.BlockSpec((CH * negs, LANE), lambda i, *_: (shard_of(i), 0)),
                pl.BlockSpec((1, 8, LANE), lambda i, *_: (shard_of(i), 0, 0)),
            ],
            scratch_shapes=[
                pltpu.VMEM((CH * rows, LANE), F32),
                pltpu.VMEM((BLK * CH, LANE), F32),
                pltpu.VMEM((negs, CH * LANE), BF16),
                pltpu.VMEM((negs, CH * LANE), F32),
            ] + sems,
        ),
        out_shape=[
            jax.ShapeDtypeStruct((CH, edges, LANE), F32),
            jax.ShapeDtypeStruct((CH * edges, LANE), F32),
            jax.ShapeDtypeStruct((CH * negs * shards, LANE), F32),
            jax.ShapeDtypeStruct((shards, 8, LANE), F32),
        ],
        compiler_params=params(), cost_estimate=cost(edges * negs * 3072, edges * 8192), name="scores",
    )(flags, cnt, tid, nid, *operands, q)


def tail_kernel(steps, total, blocks, dim, count, flags, cnt, tid, nid, tg_ref, neg_ref, *refs):
    step = pl.program_id(0)
    acc = refs[-1]

    @pl.when(step == 0)
    def _():
        zero_rows(acc)
        scatter_plain(nid, neg_ref, acc, nid.shape[0])

    @pl.when((step < total) & block_live(jnp.minimum(step, total - 1), steps, cnt))
    def _():
        scatter_rows(tid, step * BLK, tg_ref, acc, BLK)

    outs = refs[:-1]
    per = blocks // (2 * count)
    at = step - total

    def emit(ref):
        base = row_block(at, flags[0], blocks) * WBLK

        def body(r, carry):
            lanes = pl.ds(pl.multiple_of(r * LANE, LANE), LANE)
            wire_put(ref, lanes, dim, [chunk(acc, j, LANE, base + r * LANE) for j in range(CH)])
            return carry
        lax.fori_loop(0, WBLK // LANE, body, 0, unroll=True)

    for p, ref in enumerate(outs):
        pl.when((at >= 0) & (at // per == p))(functools.partial(emit, ref))


def tail_call(flags, cnt, tid, nid, tg, neg, rows, dim, near, count):
    edges = tid.shape[0]
    total = edges // BLK
    steps = total // cnt.shape[0]
    blocks = rows // WBLK
    per = blocks // (2 * count)
    acc = pltpu.VMEM((CH * rows, LANE), F32)
    pieces = count * (2 if near else 1)
    grid = total + pieces * per
    out_specs = [
        pl.BlockSpec((dim, WBLK), lambda i, *_, p=p: (0, clip_piece(i - total, p, per))) for p in range(pieces)]
    out_shape = [jax.ShapeDtypeStruct((dim, per * WBLK), F32)] * pieces
    scratch = [acc]
    return pl.pallas_call(
        functools.partial(tail_kernel, steps, total, blocks, dim, count),
        grid_spec=pltpu.PrefetchScalarGridSpec(
            num_scalar_prefetch=4,
            grid=(grid,),
            in_specs=[
                pl.BlockSpec((CH * BLK, LANE),
                             lambda i, flags, cnt, *_: (edge_block(jnp.minimum(i, total - 1), steps, cnt), 0)),
                pl.BlockSpec(neg.shape, lambda i, *_: (0, 0)),
            ],
            out_specs=out_specs,
            scratch_shapes=scratch,
        ),
        out_shape=out_shape,
        compiler_params=params(), cost_estimate=cost(edges * 3000, edges * 6144), name="tails",
    )(flags, cnt, tid, nid, tg, neg)


def head_kernel(steps, both, cnt, hid, rid, *refs):
    refs = list(refs)
    if both:
        tid, nid = refs.pop(0), refs.pop(0)
        tg_ref, neg_ref = refs.pop(0), refs.pop(0)
    r_ref, dq_ref, a_ref, out_hbm, racc_hbm, acc, racc, hbuf, gbuf, sem, rsem = refs
    step = pl.program_id(0)

    @pl.when(step == 0)
    def _():
        zero_rows(acc)
        zero_rows(racc)
        if both:
            scatter_plain(nid, neg_ref, acc, nid.shape[0])

    @pl.when(block_live(step, steps, cnt))
    def _():
        base = step * BLK
        for j in range(2):
            d_re, d_im = dq_ref[j], dq_ref[j + 2]
            r_re, r_im = r_ref[j], r_ref[j + 2]
            put_chunk(hbuf, j, BLK, d_re * r_re + d_im * r_im)
            put_chunk(hbuf, j + 2, BLK, d_im * r_re - d_re * r_im)
            a_re, a_im = a_ref[j], a_ref[j + 2]
            put_chunk(gbuf, j, BLK, d_re * a_re + d_im * a_im)
            put_chunk(gbuf, j + 2, BLK, d_im * a_re - d_re * a_im)

        def body(t, carry):
            e = t * GROUP
            repeat = hid[base + e]
            for g in range(0, GROUP, REL_GROUP):
                repeat = repeat | rid[base + e + g]

            def fast():
                add_group(group_rows(hid, base + e, GROUP, GROUP), e, hbuf, acc)
                for g in range(0, GROUP, REL_GROUP):
                    add_group(group_rows(rid, base + e + g, REL_GROUP, REL_GROUP), e + g, gbuf, racc)

            def slow():
                for g in range(GROUP):
                    add_one(id_row(hid, base + e, g == 0, g), e + g, hbuf, acc)
                    add_one(id_row(rid, base + e, g % REL_GROUP == 0, g), e + g, gbuf, racc)

            lax.cond((repeat & 1) == 0, fast, slow)
            return carry
        lax.fori_loop(0, BLK // GROUP, body, 0)
        if both:
            scatter_rows(tid, base, tg_ref, acc, BLK)

    @pl.when(step == pl.num_programs(0) - 1)
    def _():
        copy = pltpu.make_async_copy(acc, out_hbm, sem)
        copy.start()
        rcopy = pltpu.make_async_copy(racc, racc_hbm, rsem)
        rcopy.start()
        copy.wait()
        rcopy.wait()


def head_call(cnt, hid, rid, r, dq, a, rows, rels, tails=None):
    edges = hid.shape[0]
    steps = edges // cnt.shape[0] // BLK
    both = tails is not None
    scalars, operands, specs = [cnt, hid, rid], [], []
    if both:
        tid, nid, tg, neg = tails
        scalars += [tid, nid]
        operands = [tg, neg]
        specs = [pl.BlockSpec((CH * BLK, LANE), lambda i, cnt, *_: (edge_block(i, steps, cnt), 0)),
                 pl.BlockSpec(neg.shape, lambda i, *_: (0, 0))]
    edge_spec = pl.BlockSpec((CH, BLK, LANE), lambda i, cnt, *_: (0, edge_block(i, steps, cnt), 0))
    return pl.pallas_call(
        functools.partial(head_kernel, steps, both),
        grid_spec=pltpu.PrefetchScalarGridSpec(
            num_scalar_prefetch=len(scalars),
            grid=(edges // BLK,),
            in_specs=specs + [edge_spec] * 3,
            out_specs=[pl.BlockSpec(memory_space=pl.ANY)] * 2,
            scratch_shapes=[
                pltpu.VMEM((CH * rows, LANE), F32),
                pltpu.VMEM((CH * rels, LANE), F32),
                pltpu.VMEM((BLK * CH, LANE), F32),
                pltpu.VMEM((BLK * CH, LANE), F32),
                pltpu.SemaphoreType.DMA,
                pltpu.SemaphoreType.DMA,
            ],
        ),
        out_shape=[jax.ShapeDtypeStruct((CH * rows, LANE), F32), jax.ShapeDtypeStruct((CH * rels, LANE), F32)],
        compiler_params=params(), cost_estimate=cost(edges * 6000, edges * 8192), name="heads",
    )(*scalars, *operands, r, dq, a)


def update_kernel(dim, blocks, kinds, outs, final, count, flags, *refs):
    refs = list(refs)
    parts = {kind: [refs.pop(0) for _ in range(count)] for kind in kinds}
    ent_ref, head_ref, state_ref = refs[:3]
    if final == "late":
        refs.pop(3)
    new_ref, new_state = refs[3:5]
    wires = refs[5:]
    at = pl.program_id(0)
    per = blocks // (2 * count)
    near = flags[1]
    eye = lax.broadcasted_iota(jnp.int32, (LANE, LANE), 0) == lax.broadcasted_iota(jnp.int32, (LANE, LANE), 1)

    def run(tails, wire):
        def body(r, carry):
            base = r * LANE
            lanes = pl.ds(pl.multiple_of(base, LANE), LANE)
            grad = [chunk(head_ref, j, LANE, base) for j in range(CH)]
            if kinds:
                grad = [x + y for x, y in zip(grad, wire_get(tails, lanes, dim))]
            square = jnp.sum(sum(g * g for g in grad), axis=1, keepdims=True)
            state = jnp.sum(jnp.where(eye, state_ref[r], 0.0), axis=1, keepdims=True) + square / dim
            new_state[r] = jnp.sum(jnp.where(eye, state, 0.0), axis=0, keepdims=True)
            rate = LEARN_ENT * lax.rsqrt(state + ADA_EPS)
            new = [chunk(ent_ref, j, LANE, base) - rate * grad[j] for j in range(CH)]
            if final:
                wire_put(new_ref, lanes, dim, new)
            else:
                for j in range(CH):
                    put_chunk(new_ref, j, LANE, new[j], base)
            if wire is not None:
                wire_put(wire, lanes, dim, new)
            return carry
        lax.fori_loop(0, WBLK // LANE, body, 0, unroll=True)

    if not kinds and not outs:
        run(None, None)
        return
    for p in range(count):
        now = at // per == p
        wire = wires[p * PIECES // count] if outs else None
        if not kinds:
            pl.when(now)(functools.partial(run, None, wire))
        if "first" in kinds:
            pl.when(now)(functools.partial(run, parts["first"][p], wire))
        if "second" in kinds:
            pl.when(now & (near == 0))(functools.partial(run, parts["second"][p], wire))
        if "direct" in kinds:
            pl.when(now & (near == 1))(functools.partial(run, parts["direct"][p], wire))


def update_call(flags, ent, state, head, tails, dim, late, outs, final, done=None):
    rows = ent.shape[0] // CH
    blocks = rows // WBLK
    per = blocks // (2 * PIECES)

    def at(i, flags):
        return row_block(i + late * (blocks // 2), flags[0], blocks)

    packed = pl.BlockSpec((CH * WBLK, LANE), lambda i, flags: (at(i, flags), 0))
    state_spec = pl.BlockSpec((WBLK // LANE, 1, LANE), lambda i, flags: (at(i, flags), 0, 0))
    if isinstance(tails, dict):
        kinds = [kind for kind in tails if (kind != "first") == bool(late)]
        operands = [x for kind in kinds for x in tails[kind]]
        pieces = len(tails[kinds[0]])
        specs = wire_in_specs(kinds, dim, blocks, late * (blocks // 2), pieces)
    else:
        kinds, operands, specs, pieces = [], [], [], PIECES
    first = 1 + len(operands)
    operands = operands + [ent, head, state]
    specs = specs + [packed, packed, state_spec]
    alias = {first + 2: 1}
    mode = None
    if final:
        mode = "late" if late else "own"
        new_spec = pl.BlockSpec((dim, WBLK), lambda i, flags: (0, at(i, flags)))
        new_shape = jax.ShapeDtypeStruct((dim, rows), F32)
        if late:
            operands, specs = operands + [done], specs + [pl.BlockSpec(memory_space=pl.ANY)]
            alias[first + 3] = 0
    else:
        new_spec, new_shape = packed, jax.ShapeDtypeStruct(ent.shape, F32)
        alias[first] = 0
    count = PIECES if outs else 0
    return pl.pallas_call(
        functools.partial(update_kernel, dim, blocks, kinds, outs, mode, pieces),
        grid_spec=pltpu.PrefetchScalarGridSpec(
            num_scalar_prefetch=1,
            grid=(blocks // 2,),
            in_specs=specs,
            out_specs=[new_spec, state_spec] + [
                pl.BlockSpec((dim, WBLK), lambda i, *_, p=p: (0, clip_piece(i, p, per))) for p in range(count)],
        ),
        out_shape=[new_shape, jax.ShapeDtypeStruct(state.shape, F32)]
        + [jax.ShapeDtypeStruct((dim, per * WBLK), BF16)] * count,
        input_output_aliases=alias,
        compiler_params=params(), cost_estimate=cost(rows * 2000, rows * 4500), name="update",
    )(flags, *operands)


def adagrad(param, state, grad, dim, rate):
    shape = (-1, CH, LANE)
    param, grad = param.reshape(shape), grad.reshape(shape)
    state = state + jnp.sum(grad * grad, axis=(1, 2)) / dim
    return (param - rate * grad * lax.rsqrt(state + ADA_EPS)[:, None, None]).reshape(-1, LANE), state


def solution(mesh):
    ent_size = mesh.shape["ent"]
    data_size = mesh.shape["data"]
    axes = ("data", "ent")

    def dev(j, i):
        return j * ent_size + i

    def split(pairs):
        return [(i, k) for i, k in pairs if i // 2 != k // 2], [(i, k) for i, k in pairs if i // 2 == k // 2]

    rows = range(data_size)

    def send_own(own, pairs):
        return [lax.ppermute(x, axes, [(dev(j, i), dev(j, k)) for j in rows for i, k in pairs]) for x in own]

    def send_other(other, pairs):
        near = split(pairs)[1]
        return [lax.ppermute(x, axes, [(dev(j, i), dev(j, k)) for j in rows for i, k in near]) for x in other]

    def swap(first, pairs):
        cross = split(pairs)[0]
        return [lax.ppermute(x, axes, [(dev(j, k), dev(1 - j, k)) for j in rows for _, k in cross]) for x in first]

    def device_epoch(ent_table, ada_state, rel_table, head_idx, tail_idx, rel_idx, edge_mask, neg_idx):
        dim_rows, dim = ent_table.shape
        edge_count = head_idx.shape[-1]
        idle, *ids = lax.sort(
            (1 - edge_mask[0, 0], head_idx[0, 0], tail_idx[0, 0], rel_idx[0, 0]), dimension=1, num_keys=1, is_stable=False)
        live = jnp.broadcast_to(jnp.sum(1 - idle, axis=1, keepdims=True), (ent_size, LANE))
        ids = [mark_groups(x, size) for x, size in zip(ids, (GROUP, GROUP, REL_GROUP))]
        packed = lax.all_gather(jnp.concatenate(ids + [neg_idx[0, 0] * CH, live], axis=1), "data")
        ent = pack_call(ent_table.T)
        state = ada_state.reshape(-1, 1, LANE)
        rel = pack_rows(rel_table)
        rel_state = jnp.zeros((rel_table.shape[0],), F32)
        mine, me = lax.axis_index("data"), lax.axis_index("ent")
        losses = []
        tails = ent
        fetch = [(i, i) for i in range(ent_size)]
        for s in range(ent_size):
            now = packed[:, s]
            hid, tid, rid = (now[:, i * edge_count:(i + 1) * edge_count].reshape(-1) for i in range(3))
            nid = now[:, 3 * edge_count:-LANE].reshape(-1)
            cnt = now[:, -1]
            back = [(k, i) for i, k in fetch]
            back_near = s > 0 and bool(split(back)[1])
            final = s == ent_size - 1
            nxt = [((i + s + 1) % ent_size, i) for i in range(ent_size)]
            nxt_near = bool(split(nxt)[1])

            def flags_of(pairs):
                near = [k for _, k in split(pairs)[1]]
                hit = functools.reduce(jnp.logical_or, [me == k for k in near], jnp.bool_(False))
                return jnp.stack([mine, hit.astype(jnp.int32)]).astype(jnp.int32)

            fetch_flags, back_flags = flags_of(fetch), flags_of(back)
            q, a, r = query_call(cnt, hid, rid, ent, rel)
            if s and "second" not in tails:
                rest = [lax.optimization_barrier((x, q))[0] for x in tails["first"][1:]]
                tails["first"] = tails["first"][:1] + rest
                tails["second"] = swap(tails["first"], fetch)
            dq, tg, neg, loss = main_call(fetch_flags, cnt, tid, nid, tails, q, dim_rows, dim)
            tail_grad, local = None, (tid, nid, tg, neg)
            if s:
                count = PIECES if back_near else FINE
                pieces = tail_call(fetch_flags, cnt, *local, dim_rows, dim, back_near, count)
                tail_grad, local = {"first": send_own(pieces[:count], back)}, None
                if back_near:
                    tail_grad["direct"] = send_other(pieces[count:], back)
            head_grad, rel_grad = head_call(cnt, hid, rid, r, dq, a, dim_rows, rel_table.shape[0], local)
            rel_grad = lax.psum(rel_grad, "ent")
            if s:
                ready = []
                for x in tail_grad["first"]:
                    x, head_grad = lax.optimization_barrier((x, head_grad))
                    ready.append(x)
                tail_grad["first"] = ready
                tail_grad["second"] = swap(ready, back)
            new_ent, state, *own = update_call(
                back_flags, ent, state, head_grad, tail_grad, dim, 0, not final, final)
            if not final:
                own, rel_grad = lax.optimization_barrier((own, rel_grad))
                tails = {"first": send_own(own, nxt)}
                ent, state, *other = update_call(
                    back_flags, new_ent, state, head_grad, tail_grad, dim, 1, nxt_near, False)
                early = s + 2 < ent_size
                if early:
                    lead, ent = lax.optimization_barrier((tails["first"][0], ent))
                    tails["first"][0] = lead
                else:
                    tails["first"] = [lax.optimization_barrier((x, state))[0] for x in tails["first"]]
                    tails["second"] = swap(tails["first"], nxt)
                if nxt_near:
                    tails["direct"] = send_other(other, nxt)
            else:
                new_ent, rel_grad = lax.optimization_barrier((new_ent, rel_grad))
                ent, state = update_call(
                    back_flags, ent, state, head_grad, tail_grad, dim, 1, False, True, new_ent)
            rel, rel_state = adagrad(rel, rel_state, rel_grad, dim, LEARN_REL)
            losses.append(jnp.where(mine == 0, loss[0, 0, 0], loss[1, 0, 0]) / edge_count)
            fetch = nxt
        return ent.T, state.reshape(-1), unpack_rows(rel, dim), jnp.stack(losses)[None, None, :]

    ent_spec = P(("sweep", "ent"), None)
    row_spec = P(("sweep", "ent"))
    rel_spec = P("sweep", None)
    edge_spec = P(("sweep", "ent"), "data", None, None)
    loss_spec = P(("sweep", "ent"), "data", None)
    return jax.shard_map(
        device_epoch, mesh=mesh,
        in_specs=(ent_spec, row_spec, rel_spec, edge_spec, edge_spec, edge_spec, edge_spec, edge_spec),
        out_specs=(ent_spec, row_spec, rel_spec, loss_spec),
        check_vma=False)
```
